32 devices in a mesh: row: 4 (over y, x), col: 8 (over z, core).
Axes of the slice: x: 2, y: 2, z: 4, core: 2. Of those that a mesh axis runs over, the one named last changes fastest.
Arguments:
- object_field: float32 [2, 1024, 2048], P(None, 'row', 'col'), may hold values from -5 to 5
- velocity: float32 [2, 1024, 2048], P(None, 'row', 'col'), may hold values from -5 to 5
- positions: int32 [4, 8, 1, 2], P('row', 'col'), may hold values from 0 to 128
- measured: float32 [4, 8, 1, 256, 256], P('row', 'col'), may hold values from 0 to 2
- probe: float32 [2, 256, 256], replicated, may hold values from -5 to 5
Outputs:
- object_out: float32 [2, 1024, 2048], P(None, 'row', 'col')
- velocity_out: float32 [2, 1024, 2048], P(None, 'row', 'col')
The draws below stay inside these ranges and needn't reach their ends.
All inputs are finite; a program needn't handle non-finite values.
Results may differ from the reference program's by a relative error of at most 0.00018.
Values sent between devices are 32-bit elements; how exact they have to be, the bound alone decides.
No kernel may reach another device: no remote copies, remote signals or barrier semaphores. Data moves between devices by JAX's collectives and lax.ppermute only.
A program may use at most 64 MiB of HBM per device.

```python
import math
import jax
import jax.numpy as jnp
from jax import lax

TILE = 256
P_SIZE = 256
W = 128
POS = 1
ITERS = 2
TILES_R = 4
TILES_C = 8
NY = 1024
NX = 2048
N_ROW = 4
N_COL = 8


def set_ends(array, rng, low, largest):
    dims = array.shape
    index_at = [jax.random.randint(jax.random.fold_in(rng, axis), (), 0, dims[axis]) for axis in range(len(dims))]
    array = array.at[tuple(index_at)].set(low)
    longest = dims.index(max(dims))
    index_at[longest] = (index_at[longest] + 1) % dims[longest]
    return array.at[tuple(index_at)].set(largest)


def shard_levels(key, dims, shards, low, largest):
    def one(position, shards_of):
        draws = jax.random.uniform(jax.random.fold_in(jax.random.fold_in(key, 6), position), (shards_of,), jnp.float32, low / len(shards), largest / len(shards))
        return jnp.repeat(jnp.exp(draws), dims[position] // shards_of).reshape((-1,) + (1,) * (len(dims) - position - 1))

    factor_of = one(*shards[0])
    for cut in shards[1:]:
        factor_of = factor_of * one(*cut)
    return factor_of


def normal_values(own_key, extent, deviation, most, shards=(), held_as=jnp.bfloat16):
    entries = jax.random.normal(own_key, extent, jnp.float32) * deviation
    if len(shards) > 0:
        entries = shard_levels(own_key, extent, shards, -0.22, 0.18) * entries
    return jnp.clip(entries, min=-most, max=most).astype(held_as)


def setup_inputs(seed: int = 0) -> dict:
    keys = jax.random.split(jax.random.key(seed), 6)
    object_field = normal_values(keys[0], (2, NY, NX), 0.7, 5.0, ((1, 4), (2, 8)), jnp.float32)
    velocity = normal_values(keys[1], (2, NY, NX), 0.5, 5.0, ((1, 4), (2, 8)), jnp.float32)
    positions = set_ends(jax.random.randint(keys[2], (TILES_R, TILES_C, POS, 2), 0, TILE + W - P_SIZE + 1), jax.random.fold_in(keys[2], 1), 0, TILE + W - P_SIZE).astype(jnp.int32)
    measured = jnp.clip(2.0 * jax.random.uniform(keys[3], (TILES_R, TILES_C, POS, P_SIZE, P_SIZE), jnp.float32) ** shard_levels(keys[3], (TILES_R, TILES_C, POS, P_SIZE, P_SIZE), ((0, 4), (1, 8)), -0.2, 0.2), 0.0, 2.0)
    probe = normal_values(keys[4], (2, P_SIZE, P_SIZE), 0.7, 5.0, (), jnp.float32)
    return {"object_field": object_field, "velocity": velocity, "positions": positions, "measured": measured, "probe": probe}


step_size = 0.1
momentum_rate = 0.8

def fourier_tables(length):
    index = jnp.arange(length, dtype=jnp.int32)
    phase = index[:, None] * index[None, :] % length
    angle = -2.0 * math.pi * phase.astype(jnp.float32) / length
    scale = 1.0 / math.sqrt(length)
    return (jnp.cos(angle) * scale, jnp.sin(angle) * scale)

def left_product(table_re, table_im, field_re, field_im):
    hp = lax.Precision.HIGHEST

    def mult(a, b):
        return jnp.einsum('jk,pkl->pjl', a, b, precision=hp)
    return (mult(table_re, field_re) - mult(table_im, field_im), mult(table_re, field_im) + mult(table_im, field_re))

def right_product(field_re, field_im, table_re, table_im):
    hp = lax.Precision.HIGHEST

    def mult(a, b):
        return jnp.einsum('pjk,kl->pjl', a, b, precision=hp)
    return (mult(field_re, table_re) - mult(field_im, table_im), mult(field_re, table_im) + mult(field_im, table_re))

def patch_gradients(patches, intensity, probe, table_re, table_im):
    probe_re = probe[0][None]
    probe_im = probe[1][None]
    exit_re = probe_re * patches[0] - probe_im * patches[1]
    exit_im = probe_re * patches[1] + probe_im * patches[0]
    far_re, far_im = left_product(table_re, table_im, exit_re, exit_im)
    far_re, far_im = right_product(far_re, far_im, table_re, table_im)
    misfit = far_re * far_re + far_im * far_im - intensity
    back_re, back_im = (misfit * far_re, misfit * far_im)
    back_re, back_im = left_product(table_re, -table_im, back_re, back_im)
    back_re, back_im = right_product(back_re, back_im, table_re, -table_im)
    out_re = probe_re * back_re + probe_im * back_im
    out_im = probe_re * back_im - probe_im * back_re
    return jnp.stack([out_re, out_im])

def reference(object_field, velocity, positions, measured, probe):
    table_re, table_im = fourier_tables(P_SIZE)
    count = N_ROW * N_COL * POS
    for sweep in range(ITERS):
        extended = jnp.pad(object_field, ((0, 0), (0, W), (0, W)))

        def add_window(number, gradient):
            number = number.astype(jnp.int32)
            tile_row = number // (N_COL * POS)
            tile_col = number // POS % N_COL
            which = number % POS
            top = (tile_row * TILE + positions[tile_row, tile_col, which, 0]).astype(jnp.int32)
            leftmost = (tile_col * TILE + positions[tile_row, tile_col, which, 1]).astype(jnp.int32)
            zero = jnp.zeros((), jnp.int32)
            patch = lax.dynamic_slice(extended, (zero, top, leftmost), (2, P_SIZE, P_SIZE))
            intensity = measured[tile_row, tile_col, which][None]
            piece = patch_gradients(patch[:, None], intensity, probe, table_re, table_im)[:, 0]
            current = lax.dynamic_slice(gradient, (zero, top, leftmost), (2, P_SIZE, P_SIZE))
            return lax.dynamic_update_slice(gradient, current + piece, (zero, top, leftmost))
        gradient = lax.fori_loop(0, count, add_window, jnp.zeros_like(extended))
        gradient = gradient[:, :NY, :NX]
        velocity = momentum_rate * velocity + gradient
        object_field = object_field - step_size * velocity
    return (object_field, velocity)
```

```python
import math

import jax
import jax.numpy as jnp
import numpy as np
from jax import lax
from jax.experimental import pallas as pl
from jax.experimental.pallas import tpu as pltpu
from jax.sharding import PartitionSpec as P

P_SIZE = 256
W = 128
ITERS = 2

step_size = 0.1
momentum_rate = 0.8

VMEM = pl.BlockSpec(memory_space=pltpu.VMEM)
SMEM = pl.BlockSpec(memory_space=pltpu.SMEM)


def shifted(value, row_steps, col_steps):
    rows, cols = lax.axis_size("row"), lax.axis_size("col")
    pairs = []
    for r in range(rows):
        for c in range(cols):
            to_r, to_c = r + row_steps, c + col_steps
            if 0 <= to_r < rows and 0 <= to_c < cols:
                pairs.append((r * cols + c, to_r * cols + to_c))
    return lax.ppermute(value, ("row", "col"), pairs)


def halves(x):
    high = x.astype(jnp.bfloat16)
    return high, (x - high.astype(jnp.float32)).astype(jnp.bfloat16)


def transform_tables():
    index = np.arange(P_SIZE)
    angle = -2.0 * math.pi * (index[:, None] * index[None, :] % P_SIZE) / P_SIZE
    scale = 1.0 / math.sqrt(P_SIZE)
    parts = []
    for table in (np.cos(angle) * scale, np.sin(angle) * scale):
        table = table.astype(np.float32)
        high = table.astype(jnp.bfloat16)
        low = (table - high.astype(np.float32)).astype(jnp.bfloat16)
        parts += [high, low]
    return parts


def left_tables():
    c_hi, c_lo, s_hi, s_lo = transform_tables()

    def block(c, s):
        return np.concatenate(
            [np.concatenate([c, -s], axis=1), np.concatenate([s, c], axis=1)], axis=0
        )

    def block_conj(c, s):
        return block(c, -s)

    forward = np.stack([block(c_hi, s_hi), block(c_lo, s_lo)])
    inverse = np.stack([block_conj(c_hi, s_hi), block_conj(c_lo, s_lo)])
    return forward, inverse


def roll_kernel(pos_ref, probe_ref, out_ref):
    p0 = pos_ref[0]
    p1 = pos_ref[1]
    for part in range(2):
        x = pltpu.roll(probe_ref[part], p0, 0)
        out_ref[part] = pltpu.roll(x, p1, 1)


def dot(a, b):
    return jnp.dot(a, b, preferred_element_type=jnp.float32)


def left(table, x):
    x_hi, x_lo = halves(x)
    return dot(table[0], x_hi) + dot(table[0], x_lo) + dot(table[1], x_hi)


def right(x, table):
    x_hi, x_lo = halves(x)
    return dot(x_hi, table[0]) + dot(x_lo, table[0]) + dot(x_hi, table[1])


def window_kernel(
    pos_ref, own_ref, lower_ref, beside_ref, corner_ref, probe_ref, meas_ref, fwd_ref, inv_ref,
    g_own_ref, g_down_ref, g_right_ref, g_diag_ref,
):
    p0 = pos_ref[0]
    p1 = pos_ref[1]
    n, w = P_SIZE, W
    row_id = lax.broadcasted_iota(jnp.int32, (n, n), 0)
    col_id = lax.broadcasted_iota(jnp.int32, (n, n), 1)
    below = row_id < p0
    beyond = col_id < p1
    patch = []
    for part in range(2):
        top = jnp.where(below[:w], lower_ref[part], own_ref[part, :w])
        bottom = own_ref[part, w:]
        side = beside_ref[part]
        top_side = jnp.where(below[:w, :w], corner_ref[part], side[:w])
        top_left = jnp.where(beyond[:w, :w], top_side, top[:, :w])
        bottom_left = jnp.where(beyond[w:, :w], side[w:], bottom[:, :w])
        patch.append(
            jnp.concatenate(
                [
                    jnp.concatenate([top_left, top[:, w:]], axis=1),
                    jnp.concatenate([bottom_left, bottom[:, w:]], axis=1),
                ],
                axis=0,
            )
        )
    pr, pi = probe_ref[0], probe_ref[1]
    exit_re = pr * patch[0] - pi * patch[1]
    exit_im = pr * patch[1] + pi * patch[0]
    y = left(fwd_ref, jnp.concatenate([exit_re, exit_im], axis=0))
    z = right(jnp.concatenate([y[:n], y[n:]], axis=1), inv_ref)
    far_re, far_im = z[:, :n], z[:, n:]
    misfit = far_re * far_re + far_im * far_im - meas_ref[...]
    y = left(inv_ref, jnp.concatenate([misfit * far_re, misfit * far_im], axis=0))
    z = right(jnp.concatenate([y[:n], y[n:]], axis=1), fwd_ref)
    back_re, back_im = z[:, :n], z[:, n:]
    out = (pr * back_re + pi * back_im, pr * back_im - pi * back_re)
    for part in range(2):
        g = out[part]
        g_own_ref[part] = jnp.where(jnp.logical_or(below, beyond), 0.0, g)
        g_down_ref[part] = jnp.where(jnp.logical_and(below, ~beyond)[:w], g[:w], 0.0)
        g_right_ref[part] = jnp.where(jnp.logical_and(~below, beyond)[:, :w], g[:, :w], 0.0)
        g_diag_ref[part] = jnp.where(jnp.logical_and(below, beyond)[:w, :w], g[:w, :w], 0.0)


def update_kernel(obj_ref, vel_ref, g_ref, above_ref, before_ref, diag_ref, obj_out, vel_out):
    w = W
    for part in range(2):
        g = g_ref[part]
        top = g[:w] + above_ref[part]
        side = before_ref[part]
        top_left = top[:, :w] + side[:w] + diag_ref[part]
        bottom_left = g[w:, :w] + side[w:]
        g = jnp.concatenate(
            [
                jnp.concatenate([top_left, top[:, w:]], axis=1),
                jnp.concatenate([bottom_left, g[w:, w:]], axis=1),
            ],
            axis=0,
        )
        vel = momentum_rate * vel_ref[part] + g
        vel_out[part] = vel
        obj_out[part] = obj_ref[part] - step_size * vel


def shape(*dims):
    return jax.ShapeDtypeStruct(dims, jnp.float32)


def on_device(object_field, velocity, positions, measured, probe):
    n, w = P_SIZE, W
    forward, inverse = left_tables()
    forward, inverse = jnp.asarray(forward), jnp.asarray(inverse)
    offsets = positions[0, 0, 0]
    intensity = measured[0, 0, 0]
    params = pltpu.CompilerParams(vmem_limit_bytes=24 * 1024 * 1024)
    roll = pl.pallas_call(
        roll_kernel,
        out_shape=shape(2, n, n),
        in_specs=[SMEM, VMEM],
        out_specs=VMEM,
        compiler_params=params,
        cost_estimate=pl.CostEstimate(flops=10**8, bytes_accessed=10**6, transcendentals=0),
        name="roll_probe",
    )
    window = pl.pallas_call(
        window_kernel,
        out_shape=(shape(2, n, n), shape(2, w, n), shape(2, n, w), shape(2, w, w)),
        in_specs=[SMEM] + [VMEM] * 8,
        out_specs=(VMEM,) * 4,
        compiler_params=params,
        cost_estimate=pl.CostEstimate(flops=2 * 10**9, bytes_accessed=4 * 10**6, transcendentals=0),
        name="window",
    )
    update = pl.pallas_call(
        update_kernel,
        out_shape=(shape(2, n, n), shape(2, n, n)),
        in_specs=[VMEM] * 6,
        out_specs=(VMEM,) * 2,
        compiler_params=params,
        cost_estimate=pl.CostEstimate(flops=10**6, bytes_accessed=4 * 10**6, transcendentals=0),
        name="update",
    )
    turned = roll(offsets, probe)
    for sweep in range(ITERS):
        lower = shifted(object_field[:, :w, :], -1, 0)
        corner = shifted(object_field[:, :w, :w], -1, -1)
        beside = shifted(object_field[:, :, :w], 0, -1)
        own, down, right_part, diag = window(
            offsets, object_field, lower, beside, corner, turned, intensity, forward, inverse
        )
        above = shifted(down, 1, 0)
        from_corner = shifted(diag, 1, 1)
        before = shifted(right_part, 0, 1)
        object_field, velocity = update(object_field, velocity, own, above, before, from_corner)
    return (object_field, velocity)


def solution(mesh):
    placed = (
        P(None, "row", "col"),
        P(None, "row", "col"),
        P("row", "col", None, None),
        P("row", "col", None, None, None),
        P(),
    )
    return jax.shard_map(
        on_device,
        mesh=mesh,
        in_specs=placed,
        out_specs=(P(None, "row", "col"), P(None, "row", "col")),
        check_vma=False,
    )
```

```python
import math

import jax
import jax.numpy as jnp
import numpy as np
from jax import lax
from jax.experimental import pallas as pl
from jax.experimental.pallas import tpu as pltpu
from jax.sharding import PartitionSpec as P


P_SIZE = 256
W = 128
ITERS = 2

step_size = 0.1
momentum_rate = 0.8

VMEM = pl.BlockSpec(memory_space=pltpu.VMEM)
SMEM = pl.BlockSpec(memory_space=pltpu.SMEM)
N = P_SIZE
H = P_SIZE // 2


def shifted(value, row_steps, col_steps):
    rows, cols = lax.axis_size("row"), lax.axis_size("col")
    pairs = []
    for r in range(rows):
        for c in range(cols):
            to_r, to_c = r + row_steps, c + col_steps
            if 0 <= to_r < rows and 0 <= to_c < cols:
                pairs.append((r * cols + c, to_r * cols + to_c))
    return lax.ppermute(value, ("row", "col"), pairs)


def constants():
    index = np.arange(H)
    angle = -2.0 * math.pi * (index[:, None] * index[None, :] % H) / H
    scale = 1.0 / math.sqrt(P_SIZE)
    c, s = np.cos(angle) * scale, np.sin(angle) * scale
    pairs = []
    for block in (np.block([[c, s], [-s, c]]), np.block([[c, -s], [s, c]])):
        block = block.astype(np.float32)
        high = block.astype(jnp.bfloat16)
        pairs += [high, (block - high.astype(np.float32)).astype(jnp.bfloat16)]
    turn = -2.0 * math.pi * index / P_SIZE
    twiddle = np.stack([np.cos(turn), np.sin(turn)]).astype(np.float32)
    along_cols = np.broadcast_to(twiddle[:, None, :], (2, 8, H))
    along_rows = np.broadcast_to(twiddle[:, :, None], (2, H, H))
    return np.stack(pairs), np.ascontiguousarray(along_cols), np.ascontiguousarray(along_rows)


def halves(x):
    high = x.astype(jnp.bfloat16)
    return high, (x - high.astype(jnp.float32)).astype(jnp.bfloat16)


def dot(a, b):
    return jnp.dot(a, b, preferred_element_type=jnp.float32)


def times(a, b):
    return dot(a[0], b[0]) + dot(a[0], b[1]) + dot(a[1], b[0])


def quads(q00, q01, q10, q11):
    return jnp.concatenate(
        [jnp.concatenate([q00, q01], axis=1), jnp.concatenate([q10, q11], axis=1)], axis=0
    )


def block_transpose(x):
    return quads(x[:H, :H], x[H:, :H], x[:H, H:], x[H:, H:])


def plus(table_ref):
    return table_ref[0], table_ref[1]


def minus(table_ref):
    return table_ref[2], table_ref[3]


def prep_kernel(pos_ref, probe_ref, meas_ref, table_ref, cols_ref, rows_ref, probe_out, meas_out, table_out, cols_out, rows_out):
    p0 = pos_ref[0]
    p1 = pos_ref[1]
    for part in range(2):
        x = pltpu.roll(probe_ref[part], p0, 0)
        probe_out[part] = pltpu.roll(x, p1, 1)
    first = lax.broadcasted_iota(jnp.int32, (N, N), 0)
    second = lax.broadcasted_iota(jnp.int32, (N, N), 1)

    def evens_first(place):
        return jnp.where(place < H, 2 * place, 2 * (place - H) + 1)

    def moved(x, move):
        high, rest = halves(x)
        mid = x - high.astype(jnp.float32)
        low = (mid - rest.astype(jnp.float32)).astype(jnp.bfloat16)
        return move(high) + (move(rest) + move(low))

    rows_move = jnp.where(second == evens_first(first), 1.0, 0.0).astype(jnp.bfloat16)
    cols_move = jnp.where(first == evens_first(second), 1.0, 0.0).astype(jnp.bfloat16)
    x = moved(meas_ref[...], lambda part: dot(rows_move, part))
    meas_out[...] = moved(x, lambda part: dot(part, cols_move))
    table_out[...] = table_ref[...]
    cols_out[...] = cols_ref[...]
    rows_out[...] = rows_ref[...]


def row_stage(patch, pr, pi, table, w_ref):
    er = pr * patch[0] - pi * patch[1]
    ei = pr * patch[1] + pi * patch[0]
    wr, wi = w_ref[0, 0:1], w_ref[1, 0:1]
    dr, di = er[:, :H] - er[:, H:], ei[:, :H] - ei[:, H:]
    x = quads(
        er[:, :H] + er[:, H:], ei[:, :H] + ei[:, H:], dr * wr - di * wi, dr * wi + di * wr
    )
    return times(halves(x), table)


def back_stage(x, pr, pi, table, w_ref):
    y = times(halves(block_transpose(x)), table)
    wr, wi = w_ref[0, 0:1], w_ref[1, 0:1]
    qr, qi = y[H:, :H], y[H:, H:]
    tr, ti = qr * wr + qi * wi, qi * wr - qr * wi
    br = jnp.concatenate([y[:H, :H] + tr, y[:H, :H] - tr], axis=1)
    bi = jnp.concatenate([y[:H, H:] + ti, y[:H, H:] - ti], axis=1)
    return pr * br + pi * bi, pr * bi - pi * br


def masks(pos_ref):
    row_id = lax.broadcasted_iota(jnp.int32, (H, H), 0)
    col_id = lax.broadcasted_iota(jnp.int32, (H, H), 1)
    return row_id < pos_ref[0], col_id < pos_ref[1]


def pre_kernel(pos_ref, left_ref, right_ref, beside_ref, probe_ref, table_ref, cols_ref, y_ref):
    _, beyond = masks(pos_ref)
    patch = [
        jnp.concatenate(
            [jnp.where(beyond, beside_ref[part, H:], left_ref[part, H:]), right_ref[part, H:]], axis=1
        )
        for part in range(2)
    ]
    y_ref[...] = row_stage(patch, probe_ref[0, H:], probe_ref[1, H:], plus(table_ref), cols_ref)


def main_kernel(split, *refs):
    if split:
        (pos_ref, left_ref, right_ref, lower_ref, beside_ref, corner_ref, probe_ref, meas_ref, yb_ref,
         table_ref, cols_ref, rows_ref, own_out, d00_out, d01_out, diag_out, r00_out, xb_out) = refs
        lower = [[lower_ref[part, :, :H], lower_ref[part, :, H:]] for part in range(2)]
    else:
        (pos_ref, below_ref, left_ref, right_ref, up00_ref, up01_ref, mine01_ref, beside_ref, corner_ref,
         probe_ref, meas_ref, yb_ref, table_ref, cols_ref, rows_ref,
         own_out, down_out, diag_out, r00_out, xb_out) = refs
        scale = jnp.where(below_ref[0] > 0, step_size, 0.0)
        lower = [[up00_ref[part], up01_ref[part] - scale * mine01_ref[part]] for part in range(2)]
    below, beyond = masks(pos_ref)
    pr, pi = probe_ref[0, :H], probe_ref[1, :H]
    patch = []
    for part in range(2):
        q00 = jnp.where(
            below,
            jnp.where(beyond, corner_ref[part], lower[part][0]),
            jnp.where(beyond, beside_ref[part, :H], left_ref[part, :H]),
        )
        q01 = jnp.where(below, lower[part][1], right_ref[part, :H])
        patch.append(jnp.concatenate([q00, q01], axis=1))
    yt = row_stage(patch, pr, pi, plus(table_ref), cols_ref)
    yb = yb_ref[...]
    wr = jnp.concatenate([rows_ref[0], rows_ref[0]], axis=0)
    wi = jnp.concatenate([rows_ref[1], rows_ref[1]], axis=0)
    diff = yt - yb
    dr, di = diff[:, :H], diff[:, H:]
    odd = jnp.concatenate([dr * wr - di * wi, dr * wi + di * wr], axis=1)
    back = []
    for parity, x in enumerate((yt + yb, odd)):
        z = times(minus(table_ref), halves(block_transpose(x)))
        zr, zi = z[:H], z[H:]
        misfit = zr * zr + zi * zi - meas_ref[parity * H : (parity + 1) * H]
        g = jnp.concatenate([misfit * zr, misfit * zi], axis=0)
        back.append(times(plus(table_ref), halves(g)))
    qr, qi = back[1][:H], back[1][H:]
    wr = jnp.concatenate([rows_ref[0], rows_ref[0]], axis=1)
    wi = jnp.concatenate([rows_ref[1], rows_ref[1]], axis=1)
    turned = jnp.concatenate([qr * wr + qi * wi, qi * wr - qr * wi], axis=0)
    xb_out[...] = back[0] - turned
    out = back_stage(back[0] + turned, pr, pi, minus(table_ref), cols_ref)
    for part in range(2):
        g00, g01 = out[part][:, :H], out[part][:, H:]
        own_out[part, :, :H] = jnp.where(jnp.logical_or(below, beyond), 0.0, g00)
        own_out[part, :, H:] = jnp.where(below, 0.0, g01)
        d00 = jnp.where(jnp.logical_and(below, ~beyond), g00, 0.0)
        d01 = jnp.where(below, g01, 0.0)
        if split:
            d00_out[part] = d00
            d01_out[part] = d01
        else:
            down_out[part, :, :H] = d00
            down_out[part, :, H:] = d01
        diag_out[part] = jnp.where(jnp.logical_and(below, beyond), g00, 0.0)
        r00_out[part] = jnp.where(jnp.logical_and(~below, beyond), g00, 0.0)


def post_kernel(pos_ref, xb_ref, r00_ref, probe_ref, table_ref, cols_ref, own_out, right_out):
    _, beyond = masks(pos_ref)
    out = back_stage(xb_ref[...], probe_ref[0, H:], probe_ref[1, H:], minus(table_ref), cols_ref)
    for part in range(2):
        g10, g11 = out[part][:, :H], out[part][:, H:]
        own_out[part, :, :H] = jnp.where(beyond, 0.0, g10)
        own_out[part, :, H:] = g11
        right_out[part, :H] = r00_ref[part]
        right_out[part, H:] = jnp.where(beyond, g10, 0.0)


def stepped(obj, vel, g):
    vel = momentum_rate * vel + g
    return obj - step_size * vel, vel


def ahead_kernel(right_ref, vel_ref, own_ref, up_out):
    for part in range(2):
        up_out[part], _ = stepped(right_ref[part, :H], vel_ref[part, :H, H:], own_ref[part, :, H:])


def left_update_kernel(left_ref, vel_ref, top_ref, bottom_ref, d00_ref, before_ref, diag_ref, obj_out, q00_out, vel_out):
    for part in range(2):
        g00 = (top_ref[part, :, :H] + d00_ref[part]) + (before_ref[part, :H] + diag_ref[part])
        g10 = bottom_ref[part, :, :H] + before_ref[part, H:]
        obj, vel = stepped(left_ref[part, :H], vel_ref[part, :H, :H], g00)
        obj_out[part, :H] = obj
        q00_out[part] = obj
        vel_out[part, :H] = vel
        obj_out[part, H:], vel_out[part, H:] = stepped(left_ref[part, H:], vel_ref[part, H:, :H], g10)


def right_update_kernel(right_ref, vel_ref, top_ref, bottom_ref, d01_ref, obj_out, vel_out):
    for part in range(2):
        g01 = top_ref[part, :, H:] + d01_ref[part]
        obj_out[part, :H], vel_out[part, :H] = stepped(right_ref[part, :H], vel_ref[part, :H, H:], g01)
        obj_out[part, H:], vel_out[part, H:] = stepped(
            right_ref[part, H:], vel_ref[part, H:, H:], bottom_ref[part, :, H:]
        )


def final_kernel(left_ref, right_ref, vl_ref, vr_ref, top_ref, bottom_ref, above_ref, before_ref, diag_ref, obj_out, vel_out):
    for part in range(2):
        g00 = (top_ref[part, :, :H] + above_ref[part, :, :H]) + (before_ref[part, :H] + diag_ref[part])
        g01 = top_ref[part, :, H:] + above_ref[part, :, H:]
        g10 = bottom_ref[part, :, :H] + before_ref[part, H:]
        g11 = bottom_ref[part, :, H:]
        for rows, g_left, g_right in ((slice(0, H), g00, g01), (slice(H, N), g10, g11)):
            obj_out[part, rows, :H], vel_out[part, rows, :H] = stepped(left_ref[part, rows], vl_ref[part, rows], g_left)
            obj_out[part, rows, H:], vel_out[part, rows, H:] = stepped(right_ref[part, rows], vr_ref[part, rows], g_right)


def shape(*dims, dtype=jnp.float32):
    return jax.ShapeDtypeStruct(dims, dtype)


def kernel(body, name, flops, scalars, arrays, outs):
    return pl.pallas_call(
        body,
        out_shape=outs,
        in_specs=[SMEM] * scalars + [VMEM] * arrays,
        out_specs=(VMEM,) * len(outs),
        compiler_params=pltpu.CompilerParams(vmem_limit_bytes=16 * 1024 * 1024),
        cost_estimate=pl.CostEstimate(flops=flops, bytes_accessed=10**6, transcendentals=0),
        name=name,
    )


def on_device(object_field, velocity, positions, measured, probe):
    tables, along_cols, along_rows = (jnp.asarray(x) for x in constants())
    offsets = positions[0, 0, 0]
    intensity = measured[0, 0, 0]
    has_below = (lax.axis_index("row") < lax.axis_size("row") - 1).astype(jnp.int32).reshape(1)
    half, strip, quad, rows = shape(2, N, H), shape(2, H, N), shape(2, H, H), shape(N, N)

    left, right = object_field[:, :, :H], object_field[:, :, H:]
    lower = shifted(object_field[:, :H, :], -1, 0)
    corner = shifted(object_field[:, :H, :H], -1, -1)
    beside = shifted(left, 0, -1)
    turned, intensity, tables, along_cols, along_rows = kernel(
        prep_kernel, "prep", 10**8, 1, 5,
        (shape(2, N, N), rows, shape(4, N, N, dtype=jnp.bfloat16), shape(2, 8, H), shape(2, H, H)),
    )(offsets, probe, intensity, tables, along_cols, along_rows)
    pre = kernel(pre_kernel, "pre", 10**8, 1, 6, (rows,))
    post = kernel(post_kernel, "post", 10**8, 1, 5, (strip, half))

    (yb,) = pre(offsets, left, right, beside, turned, tables, along_cols)
    top, d00, d01, diag, r00, xb = kernel(
        lambda *refs: main_kernel(True, *refs), "main_first", 10**9, 1, 11, (strip, quad, quad, quad, quad, rows)
    )(offsets, left, right, lower, beside, corner, turned, intensity, yb, tables, along_cols, along_rows)
    from_above = shifted(d00, 1, 0)
    from_corner = shifted(diag, 1, 1)
    bottom, right_part = post(offsets, xb, r00, turned, tables, along_cols)
    before = shifted(right_part, 0, 1)
    above01 = shifted(d01, 1, 0)
    (ahead,) = kernel(ahead_kernel, "ahead", 10**6, 0, 3, (quad,))(right, velocity, top)
    up01 = shifted(ahead, -1, 0)

    left, q00, vel_left = kernel(left_update_kernel, "left_update", 10**6, 0, 7, (half, quad, half))(
        left, velocity, top, bottom, from_above, before, from_corner
    )
    up00 = shifted(q00, -1, 0)
    corner = shifted(q00, -1, -1)
    beside = shifted(left, 0, -1)
    right, vel_right = kernel(right_update_kernel, "right_update", 10**6, 0, 5, (half, half))(
        right, velocity, top, bottom, above01
    )

    (yb,) = pre(offsets, left, right, beside, turned, tables, along_cols)
    top, down, diag, r00, xb = kernel(
        lambda *refs: main_kernel(False, *refs), "main_last", 10**9, 2, 13, (strip, strip, quad, quad, rows)
    )(offsets, has_below, left, right, up00, up01, d01, beside, corner, turned, intensity, yb, tables, along_cols, along_rows)
    above = shifted(down, 1, 0)
    from_corner = shifted(diag, 1, 1)
    bottom, right_part = post(offsets, xb, r00, turned, tables, along_cols)
    before = shifted(right_part, 0, 1)
    return kernel(final_kernel, "final", 10**6, 0, 9, (shape(2, N, N), shape(2, N, N)))(
        left, right, vel_left, vel_right, top, bottom, above, before, from_corner
    )


def solution(mesh):
    placed = (
        P(None, "row", "col"),
        P(None, "row", "col"),
        P("row", "col", None, None),
        P("row", "col", None, None, None),
        P(),
    )
    return jax.shard_map(
        on_device,
        mesh=mesh,
        in_specs=placed,
        out_specs=(P(None, "row", "col"), P(None, "row", "col")),
        check_vma=False,
    )
```

```python
import math

import jax
import jax.numpy as jnp
import numpy as np
from jax import lax
from jax.experimental import pallas as pl
from jax.experimental.pallas import tpu as pltpu
from jax.sharding import PartitionSpec as P


P_SIZE = 256

step_size = 0.1
momentum_rate = 0.8

VMEM = pl.BlockSpec(memory_space=pltpu.VMEM)
SMEM = pl.BlockSpec(memory_space=pltpu.SMEM)
N = P_SIZE
H = P_SIZE // 2


def shifted(value, row_steps, col_steps):
    rows, cols = lax.axis_size("row"), lax.axis_size("col")
    pairs = []
    for r in range(rows):
        for c in range(cols):
            to_r, to_c = r + row_steps, c + col_steps
            if 0 <= to_r < rows and 0 <= to_c < cols:
                pairs.append((r * cols + c, to_r * cols + to_c))
    return lax.ppermute(value, ("row", "col"), pairs)


def constants():
    index = np.arange(H)
    angle = -2.0 * math.pi * (index[:, None] * index[None, :] % H) / H
    scale = 1.0 / math.sqrt(P_SIZE)
    c, s = np.cos(angle) * scale, np.sin(angle) * scale
    pairs = []
    for block in (np.block([[c, s], [-s, c]]), np.block([[c, -s], [s, c]])):
        block = block.astype(np.float32)
        high = block.astype(jnp.bfloat16)
        pairs += [high, (block - high.astype(np.float32)).astype(jnp.bfloat16)]
    turn = -2.0 * math.pi * index / P_SIZE
    twiddle = np.stack([np.cos(turn), np.sin(turn)]).astype(np.float32)
    along_cols = np.broadcast_to(twiddle[:, None, :], (2, 8, H))
    along_rows = np.broadcast_to(twiddle[:, :, None], (2, H, H))
    return np.stack(pairs), np.ascontiguousarray(along_cols), np.ascontiguousarray(along_rows)


def halves(x):
    high = x.astype(jnp.bfloat16)
    return high, (x - high.astype(jnp.float32)).astype(jnp.bfloat16)


def dot(a, b):
    return jnp.dot(a, b, preferred_element_type=jnp.float32)


def times(a, b):
    return dot(a[0], b[0]) + dot(a[0], b[1]) + dot(a[1], b[0])


def quads(q00, q01, q10, q11):
    return jnp.concatenate(
        [jnp.concatenate([q00, q01], axis=1), jnp.concatenate([q10, q11], axis=1)], axis=0
    )


def block_transpose(x):
    return quads(x[:H, :H], x[H:, :H], x[:H, H:], x[H:, H:])


def plus(table_ref):
    return table_ref[0], table_ref[1]


def minus(table_ref):
    return table_ref[2], table_ref[3]


def unpack_kernel(obj_ref, left_out, right_out, q00_out):
    for part in range(2):
        left_out[part] = obj_ref[part, :, :H]
        right_out[part] = obj_ref[part, :, H:]
        q00_out[part] = obj_ref[part, :H, :H]


def prep_kernel(
    pos_ref, probe_hbm, meas_hbm, table_hbm, cols_hbm, rows_hbm,
    probe_out, meas_out, table_out, cols_out, rows_out, probe_ref, meas_ref, sems,
):
    copies = [
        pltpu.make_async_copy(source, target, sems.at[number])
        for number, (source, target) in enumerate(
            ((probe_hbm, probe_ref), (meas_hbm, meas_ref), (table_hbm, table_out), (cols_hbm, cols_out), (rows_hbm, rows_out))
        )
    ]
    for copy in copies:
        copy.start()
    for copy in copies:
        copy.wait()
    p0 = pos_ref[0]
    p1 = pos_ref[1]
    for part in range(2):
        x = pltpu.roll(probe_ref[part], p0, 0)
        probe_out[part] = pltpu.roll(x, p1, 1)
    first = lax.broadcasted_iota(jnp.int32, (N, N), 0)
    second = lax.broadcasted_iota(jnp.int32, (N, N), 1)

    def evens_first(place):
        return jnp.where(place < H, 2 * place, 2 * (place - H) + 1)

    def moved(x, move):
        high, rest = halves(x)
        mid = x - high.astype(jnp.float32)
        low = (mid - rest.astype(jnp.float32)).astype(jnp.bfloat16)
        return move(high) + (move(rest) + move(low))

    rows_move = jnp.where(second == evens_first(first), 1.0, 0.0).astype(jnp.bfloat16)
    cols_move = jnp.where(first == evens_first(second), 1.0, 0.0).astype(jnp.bfloat16)
    x = moved(meas_ref[...], lambda part: dot(rows_move, part))
    meas_out[...] = moved(x, lambda part: dot(part, cols_move))


def row_stage(patch, pr, pi, table, w_ref):
    er = pr * patch[0] - pi * patch[1]
    ei = pr * patch[1] + pi * patch[0]
    wr, wi = w_ref[0, 0:1], w_ref[1, 0:1]
    dr, di = er[:, :H] - er[:, H:], ei[:, :H] - ei[:, H:]
    x = quads(
        er[:, :H] + er[:, H:], ei[:, :H] + ei[:, H:], dr * wr - di * wi, dr * wi + di * wr
    )
    return times(halves(x), table)


def back_stage(x, pr, pi, table, w_ref):
    y = times(halves(block_transpose(x)), table)
    wr, wi = w_ref[0, 0:1], w_ref[1, 0:1]
    qr, qi = y[H:, :H], y[H:, H:]
    tr, ti = qr * wr + qi * wi, qi * wr - qr * wi
    br = jnp.concatenate([y[:H, :H] + tr, y[:H, :H] - tr], axis=1)
    bi = jnp.concatenate([y[:H, H:] + ti, y[:H, H:] - ti], axis=1)
    return pr * br + pi * bi, pr * bi - pi * br


def masks(pos_ref):
    row_id = lax.broadcasted_iota(jnp.int32, (H, H), 0)
    col_id = lax.broadcasted_iota(jnp.int32, (H, H), 1)
    return row_id < pos_ref[0], col_id < pos_ref[1]


def pre_kernel(pos_ref, left_ref, right_ref, beside_ref, probe_ref, table_ref, cols_ref, y_ref):
    _, beyond = masks(pos_ref)
    patch = [
        jnp.concatenate(
            [jnp.where(beyond, beside_ref[part, H:], left_ref[part, H:]), right_ref[part, H:]], axis=1
        )
        for part in range(2)
    ]
    y_ref[...] = row_stage(patch, probe_ref[0, H:], probe_ref[1, H:], plus(table_ref), cols_ref)


def main_kernel(split, *refs):
    if split:
        (pos_ref, left_ref, right_ref, lower_ref, beside_ref, corner_ref, probe_ref, meas_ref, yb_ref,
         table_ref, cols_ref, rows_ref, own_out, d00_out, d01_out, diag_out, r00_out, xb_out) = refs
        lower = [[lower_ref[part, :, :H], lower_ref[part, :, H:]] for part in range(2)]
    else:
        (pos_ref, below_ref, left_ref, right_ref, up00_ref, up01_ref, mine01_ref, beside_ref, corner_ref,
         probe_ref, meas_ref, yb_ref, table_ref, cols_ref, rows_ref,
         own_out, down_out, diag_out, r00_out, xb_out) = refs
        scale = jnp.where(below_ref[0] > 0, step_size, 0.0)
        lower = [[up00_ref[part], up01_ref[part] - scale * mine01_ref[part]] for part in range(2)]
    below, beyond = masks(pos_ref)
    pr, pi = probe_ref[0, :H], probe_ref[1, :H]
    patch = []
    for part in range(2):
        q00 = jnp.where(
            below,
            jnp.where(beyond, corner_ref[part], lower[part][0]),
            jnp.where(beyond, beside_ref[part, :H], left_ref[part, :H]),
        )
        q01 = jnp.where(below, lower[part][1], right_ref[part, :H])
        patch.append(jnp.concatenate([q00, q01], axis=1))
    yt = row_stage(patch, pr, pi, plus(table_ref), cols_ref)
    yb = yb_ref[...]
    wr = jnp.concatenate([rows_ref[0], rows_ref[0]], axis=0)
    wi = jnp.concatenate([rows_ref[1], rows_ref[1]], axis=0)
    diff = yt - yb
    dr, di = diff[:, :H], diff[:, H:]
    odd = jnp.concatenate([dr * wr - di * wi, dr * wi + di * wr], axis=1)
    back = []
    for parity, x in enumerate((yt + yb, odd)):
        z = times(minus(table_ref), halves(block_transpose(x)))
        zr, zi = z[:H], z[H:]
        misfit = zr * zr + zi * zi - meas_ref[parity * H : (parity + 1) * H]
        g = jnp.concatenate([misfit * zr, misfit * zi], axis=0)
        back.append(times(plus(table_ref), halves(g)))
    qr, qi = back[1][:H], back[1][H:]
    wr = jnp.concatenate([rows_ref[0], rows_ref[0]], axis=1)
    wi = jnp.concatenate([rows_ref[1], rows_ref[1]], axis=1)
    turned = jnp.concatenate([qr * wr + qi * wi, qi * wr - qr * wi], axis=0)
    xb_out[...] = back[0] - turned
    out = back_stage(back[0] + turned, pr, pi, minus(table_ref), cols_ref)
    for part in range(2):
        g00, g01 = out[part][:, :H], out[part][:, H:]
        own_out[part, :, :H] = jnp.where(jnp.logical_or(below, beyond), 0.0, g00)
        own_out[part, :, H:] = jnp.where(below, 0.0, g01)
        d00 = jnp.where(jnp.logical_and(below, ~beyond), g00, 0.0)
        d01 = jnp.where(below, g01, 0.0)
        if split:
            d00_out[part] = d00
            d01_out[part] = d01
        else:
            down_out[part, :, :H] = d00
            down_out[part, :, H:] = d01
        diag_out[part] = jnp.where(jnp.logical_and(below, beyond), g00, 0.0)
        r00_out[part] = jnp.where(jnp.logical_and(~below, beyond), g00, 0.0)


def post_kernel(pos_ref, xb_ref, r00_ref, probe_ref, table_ref, cols_ref, own_out, right_out):
    _, beyond = masks(pos_ref)
    out = back_stage(xb_ref[...], probe_ref[0, H:], probe_ref[1, H:], minus(table_ref), cols_ref)
    for part in range(2):
        g10, g11 = out[part][:, :H], out[part][:, H:]
        own_out[part, :, :H] = jnp.where(beyond, 0.0, g10)
        own_out[part, :, H:] = g11
        right_out[part, :H] = r00_ref[part]
        right_out[part, H:] = jnp.where(beyond, g10, 0.0)


def stepped(obj, vel, g):
    vel = momentum_rate * vel + g
    return obj - step_size * vel, vel


def ahead_kernel(right_ref, vel_ref, own_ref, up_out):
    for part in range(2):
        up_out[part], _ = stepped(right_ref[part, :H], vel_ref[part, :H, H:], own_ref[part, :, H:])


def left_update_kernel(left_ref, vel_ref, top_ref, bottom_ref, d00_ref, before_ref, diag_ref, obj_out, q00_out, vel_out):
    for part in range(2):
        g00 = (top_ref[part, :, :H] + d00_ref[part]) + (before_ref[part, :H] + diag_ref[part])
        g10 = bottom_ref[part, :, :H] + before_ref[part, H:]
        obj, vel = stepped(left_ref[part, :H], vel_ref[part, :H, :H], g00)
        obj_out[part, :H] = obj
        q00_out[part] = obj
        vel_out[part, :H] = vel
        obj_out[part, H:], vel_out[part, H:] = stepped(left_ref[part, H:], vel_ref[part, H:, :H], g10)


def right_update_kernel(right_ref, vel_ref, top_ref, bottom_ref, d01_ref, obj_out, vel_out):
    for part in range(2):
        g01 = top_ref[part, :, H:] + d01_ref[part]
        obj_out[part, :H], vel_out[part, :H] = stepped(right_ref[part, :H], vel_ref[part, :H, H:], g01)
        obj_out[part, H:], vel_out[part, H:] = stepped(
            right_ref[part, H:], vel_ref[part, H:, H:], bottom_ref[part, :, H:]
        )


def final_kernel(left_ref, right_ref, vl_ref, vr_ref, top_ref, bottom_ref, above_ref, before_ref, diag_ref, obj_out, vel_out):
    for part in range(2):
        g00 = (top_ref[part, :, :H] + above_ref[part, :, :H]) + (before_ref[part, :H] + diag_ref[part])
        g01 = top_ref[part, :, H:] + above_ref[part, :, H:]
        g10 = bottom_ref[part, :, :H] + before_ref[part, H:]
        g11 = bottom_ref[part, :, H:]
        for rows, g_left, g_right in ((slice(0, H), g00, g01), (slice(H, N), g10, g11)):
            obj_out[part, rows, :H], vel_out[part, rows, :H] = stepped(left_ref[part, rows], vl_ref[part, rows], g_left)
            obj_out[part, rows, H:], vel_out[part, rows, H:] = stepped(right_ref[part, rows], vr_ref[part, rows], g_right)


def shape(*dims, dtype=jnp.float32):
    return jax.ShapeDtypeStruct(dims, dtype)


def kernel(body, flops, scalars, arrays, outs, space=VMEM, scratch=()):
    return pl.pallas_call(
        body,
        out_shape=outs,
        in_specs=[SMEM] * scalars + [space] * arrays,
        out_specs=(VMEM,) * len(outs),
        scratch_shapes=scratch,
        compiler_params=pltpu.CompilerParams(vmem_limit_bytes=16 * 1024 * 1024),
        cost_estimate=pl.CostEstimate(flops=flops, bytes_accessed=10**6, transcendentals=0),
    )


def steps(object_field, velocity, positions, measured, probe):
    tables, along_cols, along_rows = (jnp.asarray(x) for x in constants())
    offsets = positions[0, 0, 0]
    intensity = measured[0, 0, 0]
    has_below = (lax.axis_index("row") < lax.axis_size("row") - 1).astype(jnp.int32).reshape(1)
    half, strip, quad, rows = shape(2, N, H), shape(2, H, N), shape(2, H, H), shape(N, N)

    lower = shifted(object_field[:, :H, :], -1, 0)
    left, right, q00 = kernel(unpack_kernel, 10**6, 0, 1, (half, half, quad))(object_field)
    corner = shifted(q00, -1, -1)
    beside = shifted(left, 0, -1)
    turned, intensity, tables, along_cols, along_rows = kernel(
        prep_kernel, 10**8, 1, 5,
        (shape(2, N, N), rows, shape(4, N, N, dtype=jnp.bfloat16), shape(2, 8, H), shape(2, H, H)),
        pl.BlockSpec(memory_space=pl.ANY),
        (pltpu.VMEM((2, N, N), jnp.float32), pltpu.VMEM((N, N), jnp.float32), pltpu.SemaphoreType.DMA((5,))),
    )(offsets, probe, intensity, tables, along_cols, along_rows)

    def pre(left, right, beside):
        return kernel(pre_kernel, 10**8, 1, 6, (rows,))(offsets, left, right, beside, turned, tables, along_cols)[0]

    def post(xb, r00):
        return kernel(post_kernel, 10**8, 1, 5, (strip, half))(offsets, xb, r00, turned, tables, along_cols)

    yb = pre(left, right, beside)
    top, d00, d01, diag, r00, xb = kernel(
        lambda *refs: main_kernel(True, *refs), 10**9, 1, 11, (strip, quad, quad, quad, quad, rows)
    )(offsets, left, right, lower, beside, corner, turned, intensity, yb, tables, along_cols, along_rows)
    from_above = shifted(d00, 1, 0)
    from_corner = shifted(diag, 1, 1)
    bottom, right_part = post(xb, r00)
    before = shifted(right_part, 0, 1)
    above01 = shifted(d01, 1, 0)
    (ahead,) = kernel(ahead_kernel, 10**6, 0, 3, (quad,))(right, velocity, top)
    up01 = shifted(ahead, -1, 0)

    left, q00, vel_left = kernel(left_update_kernel, 10**6, 0, 7, (half, quad, half))(
        left, velocity, top, bottom, from_above, before, from_corner
    )
    up00 = shifted(q00, -1, 0)
    corner = shifted(q00, -1, -1)
    beside = shifted(left, 0, -1)
    right, vel_right = kernel(right_update_kernel, 10**6, 0, 5, (half, half))(right, velocity, top, bottom, above01)

    yb = pre(left, right, beside)
    top, down, diag, r00, xb = kernel(
        lambda *refs: main_kernel(False, *refs), 10**9, 2, 13, (strip, strip, quad, quad, rows)
    )(offsets, has_below, left, right, up00, up01, d01, beside, corner, turned, intensity, yb, tables, along_cols, along_rows)
    above = shifted(down, 1, 0)
    from_corner = shifted(diag, 1, 1)
    bottom, right_part = post(xb, r00)
    before = shifted(right_part, 0, 1)
    return kernel(final_kernel, 10**6, 0, 9, (shape(2, N, N), shape(2, N, N)))(
        left, right, vel_left, vel_right, top, bottom, above, before, from_corner
    )


def solution(mesh):
    placed = (
        P(None, "row", "col"),
        P(None, "row", "col"),
        P("row", "col", None, None),
        P("row", "col", None, None, None),
        P(),
    )
    return jax.shard_map(
        steps,
        mesh=mesh,
        in_specs=placed,
        out_specs=(P(None, "row", "col"), P(None, "row", "col")),
        check_vma=False,
    )
```

```python
import math

import jax
import jax.numpy as jnp
from jax import lax
from jax.experimental import pallas as pl
from jax.experimental.pallas import tpu as pltpu
from jax.sharding import PartitionSpec as P


P_SIZE = 256

step_size = 0.1
momentum_rate = 0.8

VMEM = pl.BlockSpec(memory_space=pltpu.VMEM)
SMEM = pl.BlockSpec(memory_space=pltpu.SMEM)
N = P_SIZE
H = P_SIZE // 2


def shifted(value, row_steps, col_steps):
    rows, cols = lax.axis_size("row"), lax.axis_size("col")
    pairs = []
    for r in range(rows):
        for c in range(cols):
            to_r, to_c = r + row_steps, c + col_steps
            if 0 <= to_r < rows and 0 <= to_c < cols:
                pairs.append((r * cols + c, to_r * cols + to_c))
    return lax.ppermute(value, ("row", "col"), pairs)


def turns(step, length, scale):
    step = jnp.where(step > length // 2, step - length, step)
    angle = step.astype(jnp.float32) * (-2.0 * math.pi / length)
    return jnp.cos(angle) * scale, jnp.sin(angle) * scale


def halves(x):
    high = x.astype(jnp.bfloat16)
    return high, (x - high.astype(jnp.float32)).astype(jnp.bfloat16)


def dot(a, b):
    return jnp.dot(a, b, preferred_element_type=jnp.float32)


def times(a, b):
    return dot(a[0], b[0]) + dot(a[0], b[1]) + dot(a[1], b[0])


def quads(q00, q01, q10, q11):
    return jnp.concatenate(
        [jnp.concatenate([q00, q01], axis=1), jnp.concatenate([q10, q11], axis=1)], axis=0
    )


def block_transpose(x):
    return quads(x[:H, :H], x[H:, :H], x[:H, H:], x[H:, H:])


def plus(table_ref):
    return table_ref[0], table_ref[1]


def minus(table_ref):
    return table_ref[2], table_ref[3]


def unpack_kernel(obj_ref, left_out, right_out, q00_out, send_out):
    for part in range(2):
        left_out[part] = obj_ref[part, :, :H]
        send_out[part] = obj_ref[part, :, :H]
        right_out[part] = obj_ref[part, :, H:]
        q00_out[part] = obj_ref[part, :H, :H]


def prep_kernel(
    pos_ref, below_ref, probe_ref, meas_ref, probe_out, meas_out, mask_out, table_out, cols_out, rows_out
):
    p0 = pos_ref[0]
    p1 = pos_ref[1]
    row_id = lax.broadcasted_iota(jnp.int32, (H, H), 0)
    col_id = lax.broadcasted_iota(jnp.int32, (H, H), 1)
    mask_out[0] = jnp.where(row_id < p0, 1, 0)
    mask_out[1] = jnp.where(col_id < p1, 1, 0)
    mask_out[2] = jnp.full((H, H), below_ref[0], jnp.int32)
    c, s = turns(row_id * col_id & (H - 1), H, 1.0 / math.sqrt(P_SIZE))
    for number, block in enumerate((quads(c, s, -s, c), quads(c, -s, s, c))):
        table_out[2 * number], table_out[2 * number + 1] = halves(block)
    rows_out[0], rows_out[1] = turns(row_id, P_SIZE, 1.0)
    cols_out[0], cols_out[1] = turns(col_id[:8], P_SIZE, 1.0)
    for part in range(2):
        x = pltpu.roll(probe_ref[part], p0, 0)
        probe_out[part] = pltpu.roll(x, p1, 1)
    first = lax.broadcasted_iota(jnp.int32, (N, N), 0)
    second = lax.broadcasted_iota(jnp.int32, (N, N), 1)

    def evens_first(place):
        return jnp.where(place < H, 2 * place, 2 * (place - H) + 1)

    def moved(x, move):
        high, rest = halves(x)
        mid = x - high.astype(jnp.float32)
        low = (mid - rest.astype(jnp.float32)).astype(jnp.bfloat16)
        return move(high) + (move(rest) + move(low))

    rows_move = jnp.where(second == evens_first(first), 1.0, 0.0).astype(jnp.bfloat16)
    cols_move = jnp.where(first == evens_first(second), 1.0, 0.0).astype(jnp.bfloat16)
    x = moved(meas_ref[...], lambda part: dot(rows_move, part))
    meas_out[...] = moved(x, lambda part: dot(part, cols_move))


def row_stage(patch, pr, pi, table, w_ref):
    er = pr * patch[0] - pi * patch[1]
    ei = pr * patch[1] + pi * patch[0]
    wr, wi = w_ref[0, 0:1], w_ref[1, 0:1]
    dr, di = er[:, :H] - er[:, H:], ei[:, :H] - ei[:, H:]
    x = quads(
        er[:, :H] + er[:, H:], ei[:, :H] + ei[:, H:], dr * wr - di * wi, dr * wi + di * wr
    )
    return times(halves(x), table)


def back_stage(x, pr, pi, table, w_ref):
    y = times(halves(block_transpose(x)), table)
    wr, wi = w_ref[0, 0:1], w_ref[1, 0:1]
    qr, qi = y[H:, :H], y[H:, H:]
    tr, ti = qr * wr + qi * wi, qi * wr - qr * wi
    br = jnp.concatenate([y[:H, :H] + tr, y[:H, :H] - tr], axis=1)
    bi = jnp.concatenate([y[:H, H:] + ti, y[:H, H:] - ti], axis=1)
    return pr * br + pi * bi, pr * bi - pi * br


def masks(mask_ref):
    return mask_ref[0] > 0, mask_ref[1] > 0


def pre_kernel(mask_ref, left_ref, right_ref, beside_ref, probe_ref, table_ref, cols_ref, y_ref):
    _, beyond = masks(mask_ref)
    patch = [
        jnp.concatenate(
            [jnp.where(beyond, beside_ref[part, H:], left_ref[part, H:]), right_ref[part, H:]], axis=1
        )
        for part in range(2)
    ]
    y_ref[...] = row_stage(patch, probe_ref[0, H:], probe_ref[1, H:], plus(table_ref), cols_ref)


def main_kernel(form, *refs):
    split = form == "first"
    if form == "first":
        (mask_ref, left_ref, right_ref, lower_ref, beside_ref, corner_ref, probe_ref, meas_ref, yb_ref,
         table_ref, cols_ref, rows_ref, own_out, d00_out, d01_out, kept_out, diag_out, r00_out, xb_out) = refs
    elif form == "whole":
        (mask_ref, left_ref, right_ref, lower_ref, beside_ref, corner_ref, probe_ref, meas_ref, yb_ref,
         table_ref, cols_ref, rows_ref, own_out, down_out, diag_out, r00_out, xb_out) = refs
    else:
        (mask_ref, left_ref, right_ref, up00_ref, up01_ref, mine01_ref, beside_ref, corner_ref,
         probe_ref, meas_ref, yb_ref, table_ref, cols_ref, rows_ref,
         own_out, down_out, diag_out, r00_out, xb_out) = refs
        scale = mask_ref[2].astype(jnp.float32) * step_size
        lower = [[up00_ref[part], up01_ref[part] - scale * mine01_ref[part]] for part in range(2)]
    if form != "second":
        lower = [[lower_ref[part, :, :H], lower_ref[part, :, H:]] for part in range(2)]
    below, beyond = masks(mask_ref)
    pr, pi = probe_ref[0, :H], probe_ref[1, :H]
    patch = []
    for part in range(2):
        q00 = jnp.where(
            below,
            jnp.where(beyond, corner_ref[part], lower[part][0]),
            jnp.where(beyond, beside_ref[part, :H], left_ref[part, :H]),
        )
        q01 = jnp.where(below, lower[part][1], right_ref[part, :H])
        patch.append(jnp.concatenate([q00, q01], axis=1))
    yt = row_stage(patch, pr, pi, plus(table_ref), cols_ref)
    yb = yb_ref[...]
    wr = jnp.concatenate([rows_ref[0], rows_ref[0]], axis=0)
    wi = jnp.concatenate([rows_ref[1], rows_ref[1]], axis=0)
    diff = yt - yb
    dr, di = diff[:, :H], diff[:, H:]
    odd = jnp.concatenate([dr * wr - di * wi, dr * wi + di * wr], axis=1)
    back = []
    for parity, x in enumerate((yt + yb, odd)):
        z = times(minus(table_ref), halves(block_transpose(x)))
        zr, zi = z[:H], z[H:]
        misfit = zr * zr + zi * zi - meas_ref[parity * H : (parity + 1) * H]
        g = jnp.concatenate([misfit * zr, misfit * zi], axis=0)
        back.append(times(plus(table_ref), halves(g)))
    qr, qi = back[1][:H], back[1][H:]
    wr = jnp.concatenate([rows_ref[0], rows_ref[0]], axis=1)
    wi = jnp.concatenate([rows_ref[1], rows_ref[1]], axis=1)
    turned = jnp.concatenate([qr * wr + qi * wi, qi * wr - qr * wi], axis=0)
    xb_out[...] = back[0] - turned
    out = back_stage(back[0] + turned, pr, pi, minus(table_ref), cols_ref)
    for part in range(2):
        g00, g01 = out[part][:, :H], out[part][:, H:]
        own_out[part, :, :H] = jnp.where(jnp.logical_or(below, beyond), 0.0, g00)
        own_out[part, :, H:] = jnp.where(below, 0.0, g01)
        d00 = jnp.where(jnp.logical_and(below, ~beyond), g00, 0.0)
        d01 = jnp.where(below, g01, 0.0)
        if split:
            d00_out[part] = d00
            d01_out[part] = d01
            kept_out[part] = d01
        else:
            down_out[part, :, :H] = d00
            down_out[part, :, H:] = d01
        diag_out[part] = jnp.where(jnp.logical_and(below, beyond), g00, 0.0)
        r00_out[part] = jnp.where(jnp.logical_and(~below, beyond), g00, 0.0)


def post_kernel(mask_ref, xb_ref, r00_ref, probe_ref, table_ref, cols_ref, own_out, right_out):
    _, beyond = masks(mask_ref)
    out = back_stage(xb_ref[...], probe_ref[0, H:], probe_ref[1, H:], minus(table_ref), cols_ref)
    for part in range(2):
        g10, g11 = out[part][:, :H], out[part][:, H:]
        own_out[part, :, :H] = jnp.where(beyond, 0.0, g10)
        own_out[part, :, H:] = g11
        right_out[part, :H] = r00_ref[part]
        right_out[part, H:] = jnp.where(beyond, g10, 0.0)


def stepped(obj, vel, g):
    vel = momentum_rate * vel + g
    return obj - step_size * vel, vel


def ahead_kernel(right_ref, vel_ref, own_ref, up_out):
    for part in range(2):
        up_out[part], _ = stepped(right_ref[part, :H], vel_ref[part, :H, H:], own_ref[part, :, H:])


def left_update_kernel(left_ref, vel_ref, top_ref, bottom_ref, d00_ref, before_ref, diag_ref, obj_out, up_out, corner_out, send_out, vel_out):
    for part in range(2):
        g00 = (top_ref[part, :, :H] + d00_ref[part]) + (before_ref[part, :H] + diag_ref[part])
        g10 = bottom_ref[part, :, :H] + before_ref[part, H:]
        obj, vel = stepped(left_ref[part, :H], vel_ref[part, :H, :H], g00)
        obj_out[part, :H] = obj
        send_out[part, :H] = obj
        up_out[part] = obj
        corner_out[part] = obj
        vel_out[part, :H] = vel
        obj, vel = stepped(left_ref[part, H:], vel_ref[part, H:, :H], g10)
        obj_out[part, H:] = obj
        send_out[part, H:] = obj
        vel_out[part, H:] = vel


def right_update_kernel(right_ref, vel_ref, top_ref, bottom_ref, d01_ref, obj_out, vel_out):
    for part in range(2):
        g01 = top_ref[part, :, H:] + d01_ref[part]
        obj_out[part, :H], vel_out[part, :H] = stepped(right_ref[part, :H], vel_ref[part, :H, H:], g01)
        obj_out[part, H:], vel_out[part, H:] = stepped(
            right_ref[part, H:], vel_ref[part, H:, H:], bottom_ref[part, :, H:]
        )


def update_kernel(
    left_ref, right_ref, vel_ref, top_ref, bottom_ref, above_ref, before_ref, diag_ref,
    left_out, right_out, vl_out, vr_out, strip_out, corner_out, send_out,
):
    for part in range(2):
        g00 = (top_ref[part, :, :H] + above_ref[part, :, :H]) + (before_ref[part, :H] + diag_ref[part])
        g01 = top_ref[part, :, H:] + above_ref[part, :, H:]
        g10 = bottom_ref[part, :, :H] + before_ref[part, H:]
        g11 = bottom_ref[part, :, H:]
        obj, vel = stepped(left_ref[part, :H], vel_ref[part, :H, :H], g00)
        left_out[part, :H], vl_out[part, :H] = obj, vel
        strip_out[part, :, :H], corner_out[part], send_out[part, :H] = obj, obj, obj
        obj, vel = stepped(right_ref[part, :H], vel_ref[part, :H, H:], g01)
        right_out[part, :H], vr_out[part, :H], strip_out[part, :, H:] = obj, vel, obj
        obj, vel = stepped(left_ref[part, H:], vel_ref[part, H:, :H], g10)
        left_out[part, H:], vl_out[part, H:], send_out[part, H:] = obj, vel, obj
        right_out[part, H:], vr_out[part, H:] = stepped(right_ref[part, H:], vel_ref[part, H:, H:], g11)


def final_kernel(left_ref, right_ref, vl_ref, vr_ref, top_ref, bottom_ref, above_ref, before_ref, diag_ref, obj_out, vel_out):
    for part in range(2):
        g00 = (top_ref[part, :, :H] + above_ref[part, :, :H]) + (before_ref[part, :H] + diag_ref[part])
        g01 = top_ref[part, :, H:] + above_ref[part, :, H:]
        g10 = bottom_ref[part, :, :H] + before_ref[part, H:]
        g11 = bottom_ref[part, :, H:]
        for rows, g_left, g_right in ((slice(0, H), g00, g01), (slice(H, N), g10, g11)):
            obj_out[part, rows, :H], vel_out[part, rows, :H] = stepped(left_ref[part, rows], vl_ref[part, rows], g_left)
            obj_out[part, rows, H:], vel_out[part, rows, H:] = stepped(right_ref[part, rows], vr_ref[part, rows], g_right)


def shape(*dims, dtype=jnp.float32):
    return jax.ShapeDtypeStruct(dims, dtype)


def kernel(body, flops, scalars, arrays, outs):
    return pl.pallas_call(
        body,
        out_shape=outs,
        in_specs=[SMEM] * scalars + [VMEM] * arrays,
        out_specs=(VMEM,) * len(outs),
        compiler_params=pltpu.CompilerParams(vmem_limit_bytes=16 * 1024 * 1024),
        cost_estimate=pl.CostEstimate(flops=flops, bytes_accessed=10**6, transcendentals=0),
    )


AHEAD = False


def steps(object_field, velocity, positions, measured, probe):
    offsets = positions[0, 0, 0]
    intensity = measured[0, 0, 0]
    has_below = (lax.axis_index("row") < lax.axis_size("row") - 1).astype(jnp.int32).reshape(1)
    half, strip, quad, rows = shape(2, N, H), shape(2, H, N), shape(2, H, H), shape(N, N)

    lower = shifted(object_field[:, :H, :], -1, 0)
    left, right, q00, left_send = kernel(unpack_kernel, 10**6, 0, 1, (half, half, quad, half))(object_field)
    beside = shifted(left_send, 0, -1)
    corner = shifted(q00, -1, -1)
    turned, intensity, mask, tables, along_cols, along_rows = kernel(
        prep_kernel, 10**8, 2, 2,
        (
            shape(2, N, N), rows, shape(3, H, H, dtype=jnp.int32),
            shape(4, N, N, dtype=jnp.bfloat16), shape(2, 8, H), shape(2, H, H),
        ),
    )(offsets, has_below, probe, intensity)

    def pre(left, right, beside):
        return kernel(pre_kernel, 10**8, 0, 7, (rows,))(
            mask, left, right, beside, turned, tables, along_cols
        )[0]

    def main(body, outs, *arrays):
        rest = (turned, intensity, pre(arrays[0], arrays[1], arrays[-2]), tables, along_cols, along_rows)
        return kernel(body, 10**9, 0, 1 + len(arrays) + len(rest), outs)(mask, *arrays, *rest)

    def post(xb, r00):
        return kernel(post_kernel, 10**8, 0, 6, (strip, half))(mask, xb, r00, turned, tables, along_cols)

    def whole(*refs):
        main_kernel("whole", *refs)

    if AHEAD:
        top, d00, d01, kept, diag, r00, xb = main(
            lambda *refs: main_kernel("first", *refs), (strip, quad, quad, quad, quad, quad, rows),
            left, right, lower, beside, corner,
        )
        from_above = shifted(d00, 1, 0)
        from_corner = shifted(diag, 1, 1)
        bottom, right_part = post(xb, r00)
        before = shifted(right_part, 0, 1)
        above01 = shifted(d01, 1, 0)
        (ahead,) = kernel(ahead_kernel, 10**6, 0, 3, (quad,))(right, velocity, top)
        up01 = shifted(ahead, -1, 0)
        left, q00, q00_corner, left_send, vel_left = kernel(
            left_update_kernel, 10**6, 0, 7, (half, quad, quad, half, half)
        )(left, velocity, top, bottom, from_above, before, from_corner)
        up00 = shifted(q00, -1, 0)
        beside = shifted(left_send, 0, -1)
        corner = shifted(q00_corner, -1, -1)
        right, vel_right = kernel(right_update_kernel, 10**6, 0, 5, (half, half))(right, velocity, top, bottom, above01)
        top, down, diag, r00, xb = main(
            lambda *refs: main_kernel("second", *refs), (strip, strip, quad, quad, rows),
            left, right, up00, up01, kept, beside, corner,
        )
    else:
        top, down, diag, r00, xb = main(whole, (strip, strip, quad, quad, rows), left, right, lower, beside, corner)
        above = shifted(down, 1, 0)
        bottom, right_part = post(xb, r00)
        before = shifted(right_part, 0, 1)
        from_corner = shifted(diag, 1, 1)
        left, right, vel_left, vel_right, strip_send, q00, left_send = kernel(
            update_kernel, 10**6, 0, 8, (half, half, half, half, strip, quad, half)
        )(left, right, velocity, top, bottom, above, before, from_corner)
        lower = shifted(strip_send, -1, 0)
        beside = shifted(left_send, 0, -1)
        corner = shifted(q00, -1, -1)
        top, down, diag, r00, xb = main(whole, (strip, strip, quad, quad, rows), left, right, lower, beside, corner)
    above = shifted(down, 1, 0)
    bottom, right_part = post(xb, r00)
    before = shifted(right_part, 0, 1)
    from_corner = shifted(diag, 1, 1)
    return kernel(final_kernel, 10**6, 0, 9, (shape(2, N, N), shape(2, N, N)))(
        left, right, vel_left, vel_right, top, bottom, above, before, from_corner
    )


def solution(mesh):
    placed = (
        P(None, "row", "col"),
        P(None, "row", "col"),
        P("row", "col", None, None),
        P("row", "col", None, None, None),
        P(),
    )
    return jax.shard_map(
        steps,
        mesh=mesh,
        in_specs=placed,
        out_specs=(P(None, "row", "col"), P(None, "row", "col")),
        check_vma=False,
    )
```

```python
import math

import jax
import jax.numpy as jnp
from jax import lax
from jax.experimental import pallas as pl
from jax.experimental.pallas import tpu as pltpu
from jax.sharding import PartitionSpec as P


P_SIZE = 256

step_size = 0.1
momentum_rate = 0.8

VMEM = pl.BlockSpec(memory_space=pltpu.VMEM)
SMEM = pl.BlockSpec(memory_space=pltpu.SMEM)
N = P_SIZE
H = P_SIZE // 2


def shifted(value, row_steps, col_steps):
    rows, cols = lax.axis_size("row"), lax.axis_size("col")
    pairs = []
    for r in range(rows):
        for c in range(cols):
            to_r, to_c = r + row_steps, c + col_steps
            if 0 <= to_r < rows and 0 <= to_c < cols:
                pairs.append((r * cols + c, to_r * cols + to_c))
    return lax.ppermute(value, ("row", "col"), pairs)


def turns(step, length, scale):
    step = jnp.where(step > length // 2, step - length, step)
    angle = step.astype(jnp.float32) * (-2.0 * math.pi / length)
    return jnp.cos(angle) * scale, jnp.sin(angle) * scale


def halves(x):
    high = x.astype(jnp.bfloat16)
    return high, (x - high.astype(jnp.float32)).astype(jnp.bfloat16)


def dot(a, b):
    return jnp.dot(a, b, preferred_element_type=jnp.float32)


def times(a, b):
    return dot(a[0], b[0]) + dot(a[0], b[1]) + dot(a[1], b[0])


def quads(q00, q01, q10, q11):
    return jnp.concatenate(
        [jnp.concatenate([q00, q01], axis=1), jnp.concatenate([q10, q11], axis=1)], axis=0
    )


def block_transpose(x):
    return quads(x[:H, :H], x[H:, :H], x[:H, H:], x[H:, H:])


def plus(table_ref):
    return table_ref[0], table_ref[1]


def minus(table_ref):
    return table_ref[2], table_ref[3]


def unpack_kernel(obj_ref, left_out, right_out, q00_out, send_out):
    for part in range(2):
        left_out[part] = obj_ref[part, :, :H]
        send_out[part] = obj_ref[part, :, :H]
        right_out[part] = obj_ref[part, :, H:]
        q00_out[part] = obj_ref[part, :H, :H]


def prep_kernel(
    pos_ref, below_ref, beside_ref, probe_ref, meas_ref, probe_out, meas_out, mask_out, table_out, cols_out, rows_out
):
    p0 = pos_ref[0]
    p1 = pos_ref[1]
    row_id = lax.broadcasted_iota(jnp.int32, (H, H), 0)
    col_id = lax.broadcasted_iota(jnp.int32, (H, H), 1)
    mask_out[0] = jnp.where(row_id < p0, 1, 0)
    mask_out[1] = jnp.where(col_id < p1, 1, 0)
    mask_out[2] = jnp.full((H, H), below_ref[0], jnp.int32)
    mask_out[3] = jnp.full((H, H), beside_ref[0], jnp.int32)
    c, s = turns(row_id * col_id & (H - 1), H, 1.0 / math.sqrt(P_SIZE))
    for number, block in enumerate((quads(c, s, -s, c), quads(c, -s, s, c))):
        table_out[2 * number], table_out[2 * number + 1] = halves(block)
    rows_out[0], rows_out[1] = turns(row_id, P_SIZE, 1.0)
    cols_out[0], cols_out[1] = turns(col_id[:8], P_SIZE, 1.0)
    for part in range(2):
        x = pltpu.roll(probe_ref[part], p0, 0)
        probe_out[part] = pltpu.roll(x, p1, 1)
    first = lax.broadcasted_iota(jnp.int32, (N, N), 0)
    second = lax.broadcasted_iota(jnp.int32, (N, N), 1)

    def evens_first(place):
        return jnp.where(place < H, 2 * place, 2 * (place - H) + 1)

    def moved(x, move):
        high, rest = halves(x)
        mid = x - high.astype(jnp.float32)
        low = (mid - rest.astype(jnp.float32)).astype(jnp.bfloat16)
        return move(high) + (move(rest) + move(low))

    rows_move = jnp.where(second == evens_first(first), 1.0, 0.0).astype(jnp.bfloat16)
    cols_move = jnp.where(first == evens_first(second), 1.0, 0.0).astype(jnp.bfloat16)
    x = moved(meas_ref[...], lambda part: dot(rows_move, part))
    meas_out[...] = moved(x, lambda part: dot(part, cols_move))


def row_stage(patch, pr, pi, table, w_ref):
    er = pr * patch[0] - pi * patch[1]
    ei = pr * patch[1] + pi * patch[0]
    wr, wi = w_ref[0, 0:1], w_ref[1, 0:1]
    dr, di = er[:, :H] - er[:, H:], ei[:, :H] - ei[:, H:]
    x = quads(
        er[:, :H] + er[:, H:], ei[:, :H] + ei[:, H:], dr * wr - di * wi, dr * wi + di * wr
    )
    return times(halves(x), table)


def back_stage(x, pr, pi, table, w_ref):
    y = times(halves(block_transpose(x)), table)
    wr, wi = w_ref[0, 0:1], w_ref[1, 0:1]
    qr, qi = y[H:, :H], y[H:, H:]
    tr, ti = qr * wr + qi * wi, qi * wr - qr * wi
    br = jnp.concatenate([y[:H, :H] + tr, y[:H, :H] - tr], axis=1)
    bi = jnp.concatenate([y[:H, H:] + ti, y[:H, H:] - ti], axis=1)
    return pr * br + pi * bi, pr * bi - pi * br


def masks(mask_ref):
    return mask_ref[0] > 0, mask_ref[1] > 0


def pre_kernel(mask_ref, left_ref, right_ref, beside_ref, probe_ref, table_ref, cols_ref, y_ref):
    _, beyond = masks(mask_ref)
    patch = [
        jnp.concatenate(
            [jnp.where(beyond, beside_ref[part, H:], left_ref[part, H:]), right_ref[part, H:]], axis=1
        )
        for part in range(2)
    ]
    y_ref[...] = row_stage(patch, probe_ref[0, H:], probe_ref[1, H:], plus(table_ref), cols_ref)


def main_kernel(first, *refs):
    if first:
        (mask_ref, left_ref, right_ref, lower_ref, beside_ref, corner_ref, probe_ref, meas_ref, yb_ref,
         table_ref, cols_ref, rows_ref, own_out, down_out, diag_out, r00_out, xb_out, kept_out) = refs
    else:
        (mask_ref, left_ref, right_ref, up00_ref, up01_ref, kept_ref, fix_ref, diag_ref, beside_ref, corner_ref,
         probe_ref, meas_ref, yb_ref, table_ref, cols_ref, rows_ref,
         own_out, down_out, diag_out, r00_out, xb_out) = refs
        kept_scale = mask_ref[2].astype(jnp.float32) * step_size
        corner_scale = kept_scale * mask_ref[3].astype(jnp.float32)
    below, beyond = masks(mask_ref)
    pr, pi = probe_ref[0, :H], probe_ref[1, :H]
    patch = []
    for part in range(2):
        own00, beside = left_ref[part, :H], beside_ref[part, :H]
        if first:
            lower00, lower01, corner = lower_ref[part, :, :H], lower_ref[part, :, H:], corner_ref[part]
        else:
            own00 = own00 - step_size * diag_ref[part]
            beside = beside - fix_ref[part, :, H:]
            lower00 = up00_ref[part] - fix_ref[part, :, :H]
            lower01 = up01_ref[part] - kept_scale * kept_ref[part, :, H:]
            corner = corner_ref[part] - corner_scale * kept_ref[part, :, :H]
        q00 = jnp.where(below, jnp.where(beyond, corner, lower00), jnp.where(beyond, beside, own00))
        q01 = jnp.where(below, lower01, right_ref[part, :H])
        patch.append(jnp.concatenate([q00, q01], axis=1))
    yt = row_stage(patch, pr, pi, plus(table_ref), cols_ref)
    yb = yb_ref[...]
    wr = jnp.concatenate([rows_ref[0], rows_ref[0]], axis=0)
    wi = jnp.concatenate([rows_ref[1], rows_ref[1]], axis=0)
    diff = yt - yb
    dr, di = diff[:, :H], diff[:, H:]
    odd = jnp.concatenate([dr * wr - di * wi, dr * wi + di * wr], axis=1)
    back = []
    for parity, x in enumerate((yt + yb, odd)):
        z = times(minus(table_ref), halves(block_transpose(x)))
        zr, zi = z[:H], z[H:]
        misfit = zr * zr + zi * zi - meas_ref[parity * H : (parity + 1) * H]
        g = jnp.concatenate([misfit * zr, misfit * zi], axis=0)
        back.append(times(plus(table_ref), halves(g)))
    qr, qi = back[1][:H], back[1][H:]
    wr = jnp.concatenate([rows_ref[0], rows_ref[0]], axis=1)
    wi = jnp.concatenate([rows_ref[1], rows_ref[1]], axis=1)
    turned = jnp.concatenate([qr * wr + qi * wi, qi * wr - qr * wi], axis=0)
    xb_out[...] = back[0] - turned
    out = back_stage(back[0] + turned, pr, pi, minus(table_ref), cols_ref)
    for part in range(2):
        g00, g01 = out[part][:, :H], out[part][:, H:]
        own_out[part, :, :H] = jnp.where(jnp.logical_or(below, beyond), 0.0, g00)
        own_out[part, :, H:] = jnp.where(below, 0.0, g01)
        d01 = jnp.where(below, g01, 0.0)
        diag = jnp.where(jnp.logical_and(below, beyond), g00, 0.0)
        diag_out[part] = diag
        if first:
            down_out[part * H : (part + 1) * H, :H] = jnp.where(below, g00, 0.0)
            down_out[part * H : (part + 1) * H, H:] = d01
            r00_out[part] = jnp.where(beyond, g00, 0.0)
            kept_out[part, :, :H] = diag
            kept_out[part, :, H:] = d01
        else:
            down_out[part, :, :H] = jnp.where(jnp.logical_and(below, ~beyond), g00, 0.0)
            down_out[part, :, H:] = d01
            r00_out[part] = jnp.where(jnp.logical_and(~below, beyond), g00, 0.0)
    if first:
        down_out[2 * H :, :H] = mask_ref[1, :8].astype(jnp.float32)
        down_out[2 * H :, H:] = jnp.zeros((8, H), jnp.float32)


def post_kernel(first, mask_ref, xb_ref, r00_ref, probe_ref, table_ref, cols_ref, own_out, right_out):
    below, beyond = masks(mask_ref)
    out = back_stage(xb_ref[...], probe_ref[0, H:], probe_ref[1, H:], minus(table_ref), cols_ref)
    for part in range(2):
        g10, g11 = out[part][:, :H], out[part][:, H:]
        own_out[part, :, :H] = jnp.where(beyond, 0.0, g10)
        own_out[part, :, H:] = g11
        r10 = jnp.where(beyond, g10, 0.0)
        if first:
            right_out[part * N : part * N + H] = r00_ref[part]
            right_out[part * N + H : (part + 1) * N] = r10
        else:
            right_out[part, :H] = r00_ref[part]
            right_out[part, H:] = r10
    if first:
        rows = jnp.sum(below.astype(jnp.float32), axis=0, keepdims=True)
        right_out[2 * N :] = jnp.broadcast_to(rows, (8, H))


def stepped(obj, vel, g):
    vel = momentum_rate * vel + g
    return obj - step_size * vel, vel


def ahead_kernel(right_ref, vel_ref, own_ref, up_out):
    for part in range(2):
        up_out[part], _ = stepped(right_ref[part, :H], vel_ref[part, :H, H:], own_ref[part, :, H:])


def update_kernel(
    mask_ref, left_ref, right_ref, vel_ref, top_ref, bottom_ref, above_ref, before_ref,
    left_out, right_out, vl_out, vr_out, up_out, corner_out, send_out, fix_out,
):
    row_id = lax.broadcasted_iota(jnp.int32, (H, H), 0).astype(jnp.float32)
    ours_above = above_ref[2 * H : 2 * H + 1, :H] < 0.5
    ours_before = row_id >= before_ref[2 * N : 2 * N + 1]
    for part in range(2):
        above, before = above_ref[part * H : (part + 1) * H], before_ref[part * N : (part + 1) * N]
        g00 = (top_ref[part, :, :H] + jnp.where(ours_above, above[:, :H], 0.0)) + jnp.where(ours_before, before[:H], 0.0)
        g01 = top_ref[part, :, H:] + above[:, H:]
        g10 = bottom_ref[part, :, :H] + before[H:]
        g11 = bottom_ref[part, :, H:]
        obj, vel = stepped(left_ref[part, :H], vel_ref[part, :H, :H], g00)
        left_out[part, :H], vl_out[part, :H] = obj, vel
        up_out[part], corner_out[part], send_out[part, :H] = obj, obj, obj
        right_out[part, :H], vr_out[part, :H] = stepped(right_ref[part, :H], vel_ref[part, :H, H:], g01)
        obj, vel = stepped(left_ref[part, H:], vel_ref[part, H:, :H], g10)
        left_out[part, H:], vl_out[part, H:], send_out[part, H:] = obj, vel, obj
        right_out[part, H:], vr_out[part, H:] = stepped(right_ref[part, H:], vel_ref[part, H:, H:], g11)
        scale = mask_ref[2].astype(jnp.float32) * step_size
        fix_out[part, :, :H] = scale * jnp.where(ours_before, 0.0, before[:H])
        scale = mask_ref[3].astype(jnp.float32) * step_size
        fix_out[part, :, H:] = scale * jnp.where(ours_above, 0.0, above[:, :H])


def final_kernel(
    left_ref, right_ref, vl_ref, vr_ref, late_ref, top_ref, bottom_ref, above_ref, before_ref, diag_ref, obj_out, vel_out
):
    for part in range(2):
        g00 = (top_ref[part, :, :H] + above_ref[part, :, :H]) + (before_ref[part, :H] + diag_ref[part])
        g01 = top_ref[part, :, H:] + above_ref[part, :, H:]
        g10 = bottom_ref[part, :, :H] + before_ref[part, H:]
        g11 = bottom_ref[part, :, H:]
        obj = left_ref[part, :H] - step_size * late_ref[part]
        obj_out[part, :H, :H], vel_out[part, :H, :H] = stepped(obj, vl_ref[part, :H] + late_ref[part], g00)
        obj_out[part, H:, :H], vel_out[part, H:, :H] = stepped(left_ref[part, H:], vl_ref[part, H:], g10)
        for rows, g in ((slice(0, H), g01), (slice(H, N), g11)):
            obj_out[part, rows, H:], vel_out[part, rows, H:] = stepped(right_ref[part, rows], vr_ref[part, rows], g)


def shape(*dims, dtype=jnp.float32):
    return jax.ShapeDtypeStruct(dims, dtype)


def kernel(body, flops, scalars, arrays, outs):
    return pl.pallas_call(
        body,
        out_shape=outs,
        in_specs=[SMEM] * scalars + [VMEM] * arrays,
        out_specs=(VMEM,) * len(outs),
        compiler_params=pltpu.CompilerParams(vmem_limit_bytes=16 * 1024 * 1024),
        cost_estimate=pl.CostEstimate(flops=flops, bytes_accessed=10**6, transcendentals=0),
    )


def steps(object_field, velocity, positions, measured, probe):
    offsets = positions[0, 0, 0]
    intensity = measured[0, 0, 0]
    edges = [
        (lax.axis_index(axis) < lax.axis_size(axis) - 1).astype(jnp.int32).reshape(1) for axis in ("row", "col")
    ]
    half, strip, quad, rows = shape(2, N, H), shape(2, H, N), shape(2, H, H), shape(N, N)

    lower = shifted(object_field[:, :H, :], -1, 0)
    left, right, q00, left_send = kernel(unpack_kernel, 10**6, 0, 1, (half, half, quad, half))(object_field)
    beside = shifted(left_send, 0, -1)
    corner = shifted(q00, -1, -1)
    turned, intensity, mask, tables, along_cols, along_rows = kernel(
        prep_kernel, 10**8, 3, 2,
        (
            shape(2, N, N), rows, shape(4, H, H, dtype=jnp.int32),
            shape(4, N, N, dtype=jnp.bfloat16), shape(2, 8, H), shape(2, H, H),
        ),
    )(offsets, *edges, probe, intensity)

    def pre(left, right, beside):
        return kernel(pre_kernel, 10**8, 0, 7, (rows,))(
            mask, left, right, beside, turned, tables, along_cols
        )[0]

    def main(body, outs, *arrays):
        rest = (turned, intensity, pre(arrays[0], arrays[1], arrays[-2]), tables, along_cols, along_rows)
        return kernel(body, 10**9, 0, 1 + len(arrays) + len(rest), outs)(mask, *arrays, *rest)

    def post(first, sent, xb, r00):
        return kernel(lambda *refs: post_kernel(first, *refs), 10**8, 0, 6, (strip, sent))(
            mask, xb, r00, turned, tables, along_cols
        )

    top, down, diag, r00, xb, kept = main(
        lambda *refs: main_kernel(True, *refs), (strip, shape(N + 8, N), quad, quad, rows, strip),
        left, right, lower, beside, corner,
    )
    above = shifted(down, 1, 0)
    bottom, right_part = post(True, shape(2 * N + 8, H), xb, r00)
    before = shifted(right_part, 0, 1)
    late = shifted(diag, 1, 1)
    (ahead,) = kernel(ahead_kernel, 10**6, 0, 3, (quad,))(right, velocity, top)
    up01 = shifted(ahead, -1, 0)
    left, right, vel_left, vel_right, q00, q00_corner, left_send, fix = kernel(
        update_kernel, 10**6, 0, 8, (half, half, half, half, quad, quad, half, strip)
    )(mask, left, right, velocity, top, bottom, above, before)
    up00 = shifted(q00, -1, 0)
    corner = shifted(q00_corner, -1, -1)
    beside = shifted(left_send, 0, -1)
    top, down, diag, r00, xb = main(
        lambda *refs: main_kernel(False, *refs), (strip, strip, quad, quad, rows),
        left, right, up00, up01, kept, fix, late, beside, corner,
    )
    above = shifted(down, 1, 0)
    bottom, right_part = post(False, half, xb, r00)
    before = shifted(right_part, 0, 1)
    from_corner = shifted(diag, 1, 1)
    return kernel(final_kernel, 10**6, 0, 10, (shape(2, N, N), shape(2, N, N)))(
        left, right, vel_left, vel_right, late, top, bottom, above, before, from_corner
    )


def solution(mesh):
    placed = (
        P(None, "row", "col"),
        P(None, "row", "col"),
        P("row", "col", None, None),
        P("row", "col", None, None, None),
        P(),
    )
    return jax.shard_map(
        steps,
        mesh=mesh,
        in_specs=placed,
        out_specs=(P(None, "row", "col"), P(None, "row", "col")),
        check_vma=False,
    )
```

```python
import math

import jax
import jax.numpy as jnp
from jax import lax
from jax.experimental import pallas as pl
from jax.experimental.pallas import tpu as pltpu
from jax.sharding import PartitionSpec as P


P_SIZE = 256

step_size = 0.1
momentum_rate = 0.8

VMEM = pl.BlockSpec(memory_space=pltpu.VMEM)
SMEM = pl.BlockSpec(memory_space=pltpu.SMEM)
N = P_SIZE
H = P_SIZE // 2


def shifted(value, row_steps, col_steps):
    rows, cols = lax.axis_size("row"), lax.axis_size("col")
    pairs = []
    for r in range(rows):
        for c in range(cols):
            to_r, to_c = r + row_steps, c + col_steps
            if 0 <= to_r < rows and 0 <= to_c < cols:
                pairs.append((r * cols + c, to_r * cols + to_c))
    return lax.ppermute(value, ("row", "col"), pairs)


def turns(step, length, scale):
    step = jnp.where(step > length // 2, step - length, step)
    angle = step.astype(jnp.float32) * (-2.0 * math.pi / length)
    return jnp.cos(angle) * scale, jnp.sin(angle) * scale


def halves(x):
    high = x.astype(jnp.bfloat16)
    return high, (x - high.astype(jnp.float32)).astype(jnp.bfloat16)


def dot(a, b):
    return jnp.dot(a, b, preferred_element_type=jnp.float32)


def times(a, b):
    return dot(a[0], b[0]) + dot(a[0], b[1]) + dot(a[1], b[0])


def quads(q00, q01, q10, q11):
    return jnp.concatenate(
        [jnp.concatenate([q00, q01], axis=1), jnp.concatenate([q10, q11], axis=1)], axis=0
    )


def block_transpose(x):
    return quads(x[:H, :H], x[H:, :H], x[:H, H:], x[H:, H:])


def plus(table_ref):
    return table_ref[0], table_ref[1]


def minus(table_ref):
    return table_ref[2], table_ref[3]


def unpack_kernel(obj_ref, left_out, right_out, q00_out, send_out):
    for part in range(2):
        left_out[part] = obj_ref[part, :, :H]
        send_out[part] = obj_ref[part, :, :H]
        right_out[part] = obj_ref[part, :, H:]
        q00_out[part] = obj_ref[part, :H, :H]


def prep_kernel(
    pos_ref, below_ref, beside_ref, probe_ref, meas_ref, probe_out, meas_out, mask_out, table_out, cols_out, rows_out
):
    p0 = pos_ref[0]
    p1 = pos_ref[1]
    row_id = lax.broadcasted_iota(jnp.int32, (H, H), 0)
    col_id = lax.broadcasted_iota(jnp.int32, (H, H), 1)
    mask_out[0] = jnp.where(row_id < p0, 1, 0)
    mask_out[1] = jnp.where(col_id < p1, 1, 0)
    mask_out[2] = jnp.full((H, H), below_ref[0], jnp.int32)
    mask_out[3] = jnp.full((H, H), beside_ref[0], jnp.int32)
    c, s = turns(row_id * col_id & (H - 1), H, 1.0 / math.sqrt(P_SIZE))
    for number, block in enumerate((quads(c, s, -s, c), quads(c, -s, s, c))):
        table_out[2 * number], table_out[2 * number + 1] = halves(block)
    rows_out[0], rows_out[1] = turns(row_id, P_SIZE, 1.0)
    cols_out[0], cols_out[1] = turns(col_id[:8], P_SIZE, 1.0)
    for part in range(2):
        x = pltpu.roll(probe_ref[part], p0, 0)
        probe_out[part] = pltpu.roll(x, p1, 1)
    first = lax.broadcasted_iota(jnp.int32, (N, N), 0)
    second = lax.broadcasted_iota(jnp.int32, (N, N), 1)

    def evens_first(place):
        return jnp.where(place < H, 2 * place, 2 * (place - H) + 1)

    def moved(x, move):
        high, rest = halves(x)
        mid = x - high.astype(jnp.float32)
        low = (mid - rest.astype(jnp.float32)).astype(jnp.bfloat16)
        return move(high) + (move(rest) + move(low))

    rows_move = jnp.where(second == evens_first(first), 1.0, 0.0).astype(jnp.bfloat16)
    cols_move = jnp.where(first == evens_first(second), 1.0, 0.0).astype(jnp.bfloat16)
    x = moved(meas_ref[...], lambda part: dot(rows_move, part))
    meas_out[...] = moved(x, lambda part: dot(part, cols_move))


def row_stage(patch, pr, pi, table, w_ref):
    er = pr * patch[0] - pi * patch[1]
    ei = pr * patch[1] + pi * patch[0]
    wr, wi = w_ref[0, 0:1], w_ref[1, 0:1]
    dr, di = er[:, :H] - er[:, H:], ei[:, :H] - ei[:, H:]
    x = quads(
        er[:, :H] + er[:, H:], ei[:, :H] + ei[:, H:], dr * wr - di * wi, dr * wi + di * wr
    )
    return times(halves(x), table)


def back_stage(x, pr, pi, table, w_ref):
    y = times(halves(block_transpose(x)), table)
    wr, wi = w_ref[0, 0:1], w_ref[1, 0:1]
    qr, qi = y[H:, :H], y[H:, H:]
    tr, ti = qr * wr + qi * wi, qi * wr - qr * wi
    br = jnp.concatenate([y[:H, :H] + tr, y[:H, :H] - tr], axis=1)
    bi = jnp.concatenate([y[:H, H:] + ti, y[:H, H:] - ti], axis=1)
    return pr * br + pi * bi, pr * bi - pi * br


def masks(mask_ref):
    return mask_ref[0] > 0, mask_ref[1] > 0


def pre_kernel(mask_ref, left_ref, right_ref, beside_ref, probe_ref, table_ref, cols_ref, y_ref):
    _, beyond = masks(mask_ref)
    patch = [
        jnp.concatenate(
            [jnp.where(beyond, beside_ref[part, H:], left_ref[part, H:]), right_ref[part, H:]], axis=1
        )
        for part in range(2)
    ]
    y_ref[...] = row_stage(patch, probe_ref[0, H:], probe_ref[1, H:], plus(table_ref), cols_ref)


def main_kernel(first, *refs):
    if first:
        (mask_ref, left_ref, right_ref, lower_ref, beside_ref, corner_ref, probe_ref, meas_ref, yb_ref,
         table_ref, cols_ref, rows_ref, own_out, down_out, diag_out, r00_out, xb_out, kept_out) = refs
    else:
        (mask_ref, left_ref, right_ref, up_ref, kept_ref, fix_ref, diag_ref, beside_ref, corner_ref,
         probe_ref, meas_ref, yb_ref, table_ref, cols_ref, rows_ref,
         own_out, down_out, diag_out, r00_out, xb_out) = refs
        corner_scale = (mask_ref[2] * mask_ref[3]).astype(jnp.float32) * step_size
    below, beyond = masks(mask_ref)
    pr, pi = probe_ref[0, :H], probe_ref[1, :H]
    patch = []
    for part in range(2):
        own00, beside = left_ref[part, :H], beside_ref[part, :H]
        if first:
            lower00, lower01, corner = lower_ref[part, :, :H], lower_ref[part, :, H:], corner_ref[part]
        else:
            own00 = own00 - step_size * diag_ref[part]
            beside = beside - fix_ref[part, :, H:]
            lower00 = up_ref[part, :, :H] - fix_ref[part, :, :H]
            lower01 = up_ref[part, :, H:]
            corner = corner_ref[part] - corner_scale * kept_ref[part]
        q00 = jnp.where(below, jnp.where(beyond, corner, lower00), jnp.where(beyond, beside, own00))
        q01 = jnp.where(below, lower01, right_ref[part, :H])
        patch.append(jnp.concatenate([q00, q01], axis=1))
    yt = row_stage(patch, pr, pi, plus(table_ref), cols_ref)
    yb = yb_ref[...]
    wr = jnp.concatenate([rows_ref[0], rows_ref[0]], axis=0)
    wi = jnp.concatenate([rows_ref[1], rows_ref[1]], axis=0)
    diff = yt - yb
    dr, di = diff[:, :H], diff[:, H:]
    odd = jnp.concatenate([dr * wr - di * wi, dr * wi + di * wr], axis=1)
    back = []
    for parity, x in enumerate((yt + yb, odd)):
        z = times(minus(table_ref), halves(block_transpose(x)))
        zr, zi = z[:H], z[H:]
        misfit = zr * zr + zi * zi - meas_ref[parity * H : (parity + 1) * H]
        g = jnp.concatenate([misfit * zr, misfit * zi], axis=0)
        back.append(times(plus(table_ref), halves(g)))
    qr, qi = back[1][:H], back[1][H:]
    wr = jnp.concatenate([rows_ref[0], rows_ref[0]], axis=1)
    wi = jnp.concatenate([rows_ref[1], rows_ref[1]], axis=1)
    turned = jnp.concatenate([qr * wr + qi * wi, qi * wr - qr * wi], axis=0)
    xb_out[...] = back[0] - turned
    out = back_stage(back[0] + turned, pr, pi, minus(table_ref), cols_ref)
    for part in range(2):
        g00, g01 = out[part][:, :H], out[part][:, H:]
        own_out[part, :, :H] = jnp.where(jnp.logical_or(below, beyond), 0.0, g00)
        own_out[part, :, H:] = jnp.where(below, 0.0, g01)
        d01 = jnp.where(below, g01, 0.0)
        diag = jnp.where(jnp.logical_and(below, beyond), g00, 0.0)
        diag_out[part] = diag
        if first:
            down_out[part * H : (part + 1) * H, :H] = jnp.where(below, g00, 0.0)
            down_out[part * H : (part + 1) * H, H:] = d01
            r00_out[part] = jnp.where(beyond, g00, 0.0)
            kept_out[part] = diag
        else:
            down_out[part, :, :H] = jnp.where(jnp.logical_and(below, ~beyond), g00, 0.0)
            down_out[part, :, H:] = d01
            r00_out[part] = jnp.where(jnp.logical_and(~below, beyond), g00, 0.0)
    if first:
        down_out[2 * H :, :H] = mask_ref[1, :8].astype(jnp.float32)
        down_out[2 * H :, H:] = jnp.zeros((8, H), jnp.float32)


def post_kernel(first, mask_ref, xb_ref, r00_ref, probe_ref, table_ref, cols_ref, own_out, right_out):
    below, beyond = masks(mask_ref)
    out = back_stage(xb_ref[...], probe_ref[0, H:], probe_ref[1, H:], minus(table_ref), cols_ref)
    for part in range(2):
        g10, g11 = out[part][:, :H], out[part][:, H:]
        own_out[part, :, :H] = jnp.where(beyond, 0.0, g10)
        own_out[part, :, H:] = g11
        r10 = jnp.where(beyond, g10, 0.0)
        if first:
            right_out[part * N : part * N + H] = r00_ref[part]
            right_out[part * N + H : (part + 1) * N] = r10
        else:
            right_out[part, :H] = r00_ref[part]
            right_out[part, H:] = r10
    if first:
        rows = jnp.sum(below.astype(jnp.float32), axis=0, keepdims=True)
        right_out[2 * N :] = jnp.broadcast_to(rows, (8, H))


def stepped(obj, vel, g):
    vel = momentum_rate * vel + g
    return obj - step_size * vel, vel


def update_kernel(
    mask_ref, left_ref, right_ref, vel_ref, top_ref, bottom_ref, above_ref, before_ref,
    left_out, right_out, vl_out, vr_out, up_out, corner_out, send_out, fix_out,
):
    row_id = lax.broadcasted_iota(jnp.int32, (H, H), 0).astype(jnp.float32)
    ours_above = above_ref[2 * H : 2 * H + 1, :H] < 0.5
    ours_before = row_id >= before_ref[2 * N : 2 * N + 1]
    for part in range(2):
        above, before = above_ref[part * H : (part + 1) * H], before_ref[part * N : (part + 1) * N]
        g00 = (top_ref[part, :, :H] + jnp.where(ours_above, above[:, :H], 0.0)) + jnp.where(ours_before, before[:H], 0.0)
        g01 = top_ref[part, :, H:] + above[:, H:]
        g10 = bottom_ref[part, :, :H] + before[H:]
        g11 = bottom_ref[part, :, H:]
        obj, vel = stepped(left_ref[part, :H], vel_ref[part, :H, :H], g00)
        left_out[part, :H], vl_out[part, :H] = obj, vel
        up_out[part, :, :H], corner_out[part], send_out[part, :H] = obj, obj, obj
        obj, vel = stepped(right_ref[part, :H], vel_ref[part, :H, H:], g01)
        right_out[part, :H], vr_out[part, :H], up_out[part, :, H:] = obj, vel, obj
        obj, vel = stepped(left_ref[part, H:], vel_ref[part, H:, :H], g10)
        left_out[part, H:], vl_out[part, H:], send_out[part, H:] = obj, vel, obj
        right_out[part, H:], vr_out[part, H:] = stepped(right_ref[part, H:], vel_ref[part, H:, H:], g11)
        scale = mask_ref[2].astype(jnp.float32) * step_size
        fix_out[part, :, :H] = scale * jnp.where(ours_before, 0.0, before[:H])
        scale = mask_ref[3].astype(jnp.float32) * step_size
        fix_out[part, :, H:] = scale * jnp.where(ours_above, 0.0, above[:, :H])


def final_kernel(
    left_ref, right_ref, vl_ref, vr_ref, late_ref, top_ref, bottom_ref, above_ref, before_ref, diag_ref, obj_out, vel_out
):
    for part in range(2):
        g00 = (top_ref[part, :, :H] + above_ref[part, :, :H]) + (before_ref[part, :H] + diag_ref[part])
        g01 = top_ref[part, :, H:] + above_ref[part, :, H:]
        g10 = bottom_ref[part, :, :H] + before_ref[part, H:]
        g11 = bottom_ref[part, :, H:]
        obj = left_ref[part, :H] - step_size * late_ref[part]
        obj_out[part, :H, :H], vel_out[part, :H, :H] = stepped(obj, vl_ref[part, :H] + late_ref[part], g00)
        obj_out[part, H:, :H], vel_out[part, H:, :H] = stepped(left_ref[part, H:], vl_ref[part, H:], g10)
        for rows, g in ((slice(0, H), g01), (slice(H, N), g11)):
            obj_out[part, rows, H:], vel_out[part, rows, H:] = stepped(right_ref[part, rows], vr_ref[part, rows], g)


def shape(*dims, dtype=jnp.float32):
    return jax.ShapeDtypeStruct(dims, dtype)


def kernel(body, flops, scalars, arrays, outs):
    return pl.pallas_call(
        body,
        out_shape=outs,
        in_specs=[SMEM] * scalars + [VMEM] * arrays,
        out_specs=(VMEM,) * len(outs),
        compiler_params=pltpu.CompilerParams(vmem_limit_bytes=16 * 1024 * 1024),
        cost_estimate=pl.CostEstimate(flops=flops, bytes_accessed=10**6, transcendentals=0),
    )


def steps(object_field, velocity, positions, measured, probe):
    offsets = positions[0, 0, 0]
    intensity = measured[0, 0, 0]
    edges = [
        (lax.axis_index(axis) < lax.axis_size(axis) - 1).astype(jnp.int32).reshape(1) for axis in ("row", "col")
    ]
    half, strip, quad, rows = shape(2, N, H), shape(2, H, N), shape(2, H, H), shape(N, N)

    lower = shifted(object_field[:, :H, :], -1, 0)
    left, right, q00, left_send = kernel(unpack_kernel, 10**6, 0, 1, (half, half, quad, half))(object_field)
    beside = shifted(left_send, 0, -1)
    corner = shifted(q00, -1, -1)
    turned, intensity, mask, tables, along_cols, along_rows = kernel(
        prep_kernel, 10**8, 3, 2,
        (
            shape(2, N, N), rows, shape(4, H, H, dtype=jnp.int32),
            shape(4, N, N, dtype=jnp.bfloat16), shape(2, 8, H), shape(2, H, H),
        ),
    )(offsets, *edges, probe, intensity)

    def pre(left, right, beside):
        return kernel(pre_kernel, 10**8, 0, 7, (rows,))(
            mask, left, right, beside, turned, tables, along_cols
        )[0]

    def main(body, outs, *arrays):
        rest = (turned, intensity, pre(arrays[0], arrays[1], arrays[-2]), tables, along_cols, along_rows)
        return kernel(body, 10**9, 0, 1 + len(arrays) + len(rest), outs)(mask, *arrays, *rest)

    def post(first, sent, xb, r00):
        return kernel(lambda *refs: post_kernel(first, *refs), 10**8, 0, 6, (strip, sent))(
            mask, xb, r00, turned, tables, along_cols
        )

    top, down, diag, r00, xb, kept = main(
        lambda *refs: main_kernel(True, *refs), (strip, shape(N + 8, N), quad, quad, rows, quad),
        left, right, lower, beside, corner,
    )
    above = shifted(down, 1, 0)
    bottom, right_part = post(True, shape(2 * N + 8, H), xb, r00)
    before = shifted(right_part, 0, 1)
    late = shifted(diag, 1, 1)
    left, right, vel_left, vel_right, q00, q00_corner, left_send, fix = kernel(
        update_kernel, 10**6, 0, 8, (half, half, half, half, strip, quad, half, strip)
    )(mask, left, right, velocity, top, bottom, above, before)
    up00 = shifted(q00, -1, 0)
    corner = shifted(q00_corner, -1, -1)
    beside = shifted(left_send, 0, -1)
    top, down, diag, r00, xb = main(
        lambda *refs: main_kernel(False, *refs), (strip, strip, quad, quad, rows),
        left, right, up00, kept, fix, late, beside, corner,
    )
    above = shifted(down, 1, 0)
    bottom, right_part = post(False, half, xb, r00)
    before = shifted(right_part, 0, 1)
    from_corner = shifted(diag, 1, 1)
    return kernel(final_kernel, 10**6, 0, 10, (shape(2, N, N), shape(2, N, N)))(
        left, right, vel_left, vel_right, late, top, bottom, above, before, from_corner
    )


def solution(mesh):
    placed = (
        P(None, "row", "col"),
        P(None, "row", "col"),
        P("row", "col", None, None),
        P("row", "col", None, None, None),
        P(),
    )
    return jax.shard_map(
        steps,
        mesh=mesh,
        in_specs=placed,
        out_specs=(P(None, "row", "col"), P(None, "row", "col")),
        check_vma=False,
    )
```

```python
import math

import jax
import jax.numpy as jnp
from jax import lax
from jax.experimental import pallas as pl
from jax.experimental.pallas import tpu as pltpu
from jax.sharding import PartitionSpec as P


P_SIZE = 256

step_size = 0.1
momentum_rate = 0.8

VMEM = pl.BlockSpec(memory_space=pltpu.VMEM)
SMEM = pl.BlockSpec(memory_space=pltpu.SMEM)
N = P_SIZE
H = P_SIZE // 2


def shifted(value, row_steps, col_steps):
    rows, cols = lax.axis_size("row"), lax.axis_size("col")
    pairs = []
    for r in range(rows):
        for c in range(cols):
            to_r, to_c = r + row_steps, c + col_steps
            if 0 <= to_r < rows and 0 <= to_c < cols:
                pairs.append((r * cols + c, to_r * cols + to_c))
    return lax.ppermute(value, ("row", "col"), pairs)


def turns(step, length, scale):
    step = jnp.where(step > length // 2, step - length, step)
    angle = step.astype(jnp.float32) * (-2.0 * math.pi / length)
    return jnp.cos(angle) * scale, jnp.sin(angle) * scale


def halves(x):
    high = x.astype(jnp.bfloat16)
    return high, (x - high.astype(jnp.float32)).astype(jnp.bfloat16)


def dot(a, b):
    return jnp.dot(a, b, preferred_element_type=jnp.float32)


def times(a, b):
    return dot(a[0], b[0]) + dot(a[0], b[1]) + dot(a[1], b[0])


def quads(q00, q01, q10, q11):
    return jnp.concatenate(
        [jnp.concatenate([q00, q01], axis=1), jnp.concatenate([q10, q11], axis=1)], axis=0
    )


def block_transpose(x):
    return quads(x[:H, :H], x[H:, :H], x[:H, H:], x[H:, H:])


def plus(table_ref):
    return table_ref[0], table_ref[1]


def minus(table_ref):
    return table_ref[2], table_ref[3]


def unpack_kernel(obj_ref, left_out, right_out, q00_out, send_out):
    for part in range(2):
        left_out[part] = obj_ref[part, :, :H]
        send_out[part] = obj_ref[part, :, :H]
        right_out[part] = obj_ref[part, :, H:]
        q00_out[part] = obj_ref[part, :H, :H]


def prep_kernel(
    pos_ref, below_ref, beside_ref, probe_ref, meas_ref, probe_out, meas_out, mask_out, table_out, cols_out, rows_out
):
    p0 = pos_ref[0]
    p1 = pos_ref[1]
    row_id = lax.broadcasted_iota(jnp.int32, (H, H), 0)
    col_id = lax.broadcasted_iota(jnp.int32, (H, H), 1)
    mask_out[0] = jnp.where(row_id < p0, 1, 0)
    mask_out[1] = jnp.where(col_id < p1, 1, 0)
    mask_out[2] = jnp.full((H, H), below_ref[0], jnp.int32)
    mask_out[3] = jnp.full((H, H), beside_ref[0], jnp.int32)
    c, s = turns(row_id * col_id & (H - 1), H, 1.0 / math.sqrt(P_SIZE))
    for number, block in enumerate((quads(c, s, -s, c), quads(c, -s, s, c))):
        table_out[2 * number], table_out[2 * number + 1] = halves(block)
    rows_out[0], rows_out[1] = turns(row_id, P_SIZE, 1.0)
    cols_out[0], cols_out[1] = turns(col_id[:8], P_SIZE, 1.0)
    for part in range(2):
        x = pltpu.roll(probe_ref[part], p0, 0)
        probe_out[part] = pltpu.roll(x, p1, 1)
    first = lax.broadcasted_iota(jnp.int32, (N, N), 0)
    second = lax.broadcasted_iota(jnp.int32, (N, N), 1)

    def evens_first(place):
        return jnp.where(place < H, 2 * place, 2 * (place - H) + 1)

    def moved(x, move):
        high, rest = halves(x)
        mid = x - high.astype(jnp.float32)
        low = (mid - rest.astype(jnp.float32)).astype(jnp.bfloat16)
        return move(high) + (move(rest) + move(low))

    rows_move = jnp.where(second == evens_first(first), 1.0, 0.0).astype(jnp.bfloat16)
    cols_move = jnp.where(first == evens_first(second), 1.0, 0.0).astype(jnp.bfloat16)
    x = moved(meas_ref[...], lambda part: dot(rows_move, part))
    meas_out[...] = moved(x, lambda part: dot(part, cols_move))


def row_stage(patch, pr, pi, table, w_ref):
    er = pr * patch[0] - pi * patch[1]
    ei = pr * patch[1] + pi * patch[0]
    wr, wi = w_ref[0, 0:1], w_ref[1, 0:1]
    dr, di = er[:, :H] - er[:, H:], ei[:, :H] - ei[:, H:]
    x = quads(
        er[:, :H] + er[:, H:], ei[:, :H] + ei[:, H:], dr * wr - di * wi, dr * wi + di * wr
    )
    return times(halves(x), table)


def back_stage(x, pr, pi, table, w_ref):
    y = times(halves(block_transpose(x)), table)
    wr, wi = w_ref[0, 0:1], w_ref[1, 0:1]
    qr, qi = y[H:, :H], y[H:, H:]
    tr, ti = qr * wr + qi * wi, qi * wr - qr * wi
    br = jnp.concatenate([y[:H, :H] + tr, y[:H, :H] - tr], axis=1)
    bi = jnp.concatenate([y[:H, H:] + ti, y[:H, H:] - ti], axis=1)
    return pr * br + pi * bi, pr * bi - pi * br


def masks(mask_ref):
    return mask_ref[0] > 0, mask_ref[1] > 0


def pre_kernel(mask_ref, left_ref, right_ref, beside_ref, probe_ref, table_ref, cols_ref, y_ref):
    _, beyond = masks(mask_ref)
    patch = [
        jnp.concatenate(
            [jnp.where(beyond, beside_ref[part, H:], left_ref[part, H:]), right_ref[part, H:]], axis=1
        )
        for part in range(2)
    ]
    y_ref[...] = row_stage(patch, probe_ref[0, H:], probe_ref[1, H:], plus(table_ref), cols_ref)


def main_kernel(first, *refs):
    if first:
        (mask_ref, left_ref, right_ref, lower_ref, beside_ref, corner_ref, probe_ref, meas_ref, yb_ref,
         table_ref, cols_ref, rows_ref, own_out, down_out, diag_out, r00_out, xb_out, kept_out) = refs
    else:
        (mask_ref, left_ref, right_ref, up_ref, kept_ref, fix_ref, diag_ref, beside_ref, corner_ref,
         probe_ref, meas_ref, yb_ref, table_ref, cols_ref, rows_ref,
         own_out, down_out, diag_out, bottom_out, right_out) = refs
        corner_scale = (mask_ref[2] * mask_ref[3]).astype(jnp.float32) * step_size
    below, beyond = masks(mask_ref)
    pr, pi = probe_ref[0, :H], probe_ref[1, :H]
    patch = []
    for part in range(2):
        own00, beside = left_ref[part, :H], beside_ref[part, :H]
        if first:
            lower00, lower01, corner = lower_ref[part, :, :H], lower_ref[part, :, H:], corner_ref[part]
        else:
            own00 = own00 - step_size * diag_ref[part]
            beside = beside - fix_ref[part, :, H:]
            lower00 = up_ref[part, :, :H] - fix_ref[part, :, :H]
            lower01 = up_ref[part, :, H:]
            corner = corner_ref[part] - corner_scale * kept_ref[part]
        q00 = jnp.where(below, jnp.where(beyond, corner, lower00), jnp.where(beyond, beside, own00))
        q01 = jnp.where(below, lower01, right_ref[part, :H])
        patch.append(jnp.concatenate([q00, q01], axis=1))
    yt = row_stage(patch, pr, pi, plus(table_ref), cols_ref)
    yb = yb_ref[...]
    wr = jnp.concatenate([rows_ref[0], rows_ref[0]], axis=0)
    wi = jnp.concatenate([rows_ref[1], rows_ref[1]], axis=0)
    diff = yt - yb
    dr, di = diff[:, :H], diff[:, H:]
    odd = jnp.concatenate([dr * wr - di * wi, dr * wi + di * wr], axis=1)
    back = []
    for parity, x in enumerate((yt + yb, odd)):
        z = times(minus(table_ref), halves(block_transpose(x)))
        zr, zi = z[:H], z[H:]
        misfit = zr * zr + zi * zi - meas_ref[parity * H : (parity + 1) * H]
        g = jnp.concatenate([misfit * zr, misfit * zi], axis=0)
        back.append(times(plus(table_ref), halves(g)))
    qr, qi = back[1][:H], back[1][H:]
    wr = jnp.concatenate([rows_ref[0], rows_ref[0]], axis=1)
    wi = jnp.concatenate([rows_ref[1], rows_ref[1]], axis=1)
    turned = jnp.concatenate([qr * wr + qi * wi, qi * wr - qr * wi], axis=0)
    if first:
        xb_out[...] = back[0] - turned
    out = back_stage(back[0] + turned, pr, pi, minus(table_ref), cols_ref)
    for part in range(2):
        g00, g01 = out[part][:, :H], out[part][:, H:]
        own_out[part, :, :H] = jnp.where(jnp.logical_or(below, beyond), 0.0, g00)
        own_out[part, :, H:] = jnp.where(below, 0.0, g01)
        d01 = jnp.where(below, g01, 0.0)
        diag = jnp.where(jnp.logical_and(below, beyond), g00, 0.0)
        diag_out[part] = diag
        if first:
            down_out[part * H : (part + 1) * H, :H] = jnp.where(below, g00, 0.0)
            down_out[part * H : (part + 1) * H, H:] = d01
            r00_out[part] = jnp.where(beyond, g00, 0.0)
            kept_out[part] = diag
        else:
            down_out[part, :, :H] = jnp.where(jnp.logical_and(below, ~beyond), g00, 0.0)
            down_out[part, :, H:] = d01
            right_out[part, :H] = jnp.where(jnp.logical_and(~below, beyond), g00, 0.0)
    if first:
        down_out[2 * H :, :H] = mask_ref[1, :8].astype(jnp.float32)
        down_out[2 * H :, H:] = jnp.zeros((8, H), jnp.float32)
    else:
        out = back_stage(back[0] - turned, probe_ref[0, H:], probe_ref[1, H:], minus(table_ref), cols_ref)
        for part in range(2):
            g10, g11 = out[part][:, :H], out[part][:, H:]
            bottom_out[part, :, :H] = jnp.where(beyond, 0.0, g10)
            bottom_out[part, :, H:] = g11
            right_out[part, H:] = jnp.where(beyond, g10, 0.0)


def post_kernel(mask_ref, xb_ref, r00_ref, probe_ref, table_ref, cols_ref, own_out, right_out):
    below, beyond = masks(mask_ref)
    out = back_stage(xb_ref[...], probe_ref[0, H:], probe_ref[1, H:], minus(table_ref), cols_ref)
    for part in range(2):
        g10, g11 = out[part][:, :H], out[part][:, H:]
        own_out[part, :, :H] = jnp.where(beyond, 0.0, g10)
        own_out[part, :, H:] = g11
        right_out[part * N : part * N + H] = r00_ref[part]
        right_out[part * N + H : (part + 1) * N] = jnp.where(beyond, g10, 0.0)
    rows = jnp.sum(below.astype(jnp.float32), axis=0, keepdims=True)
    right_out[2 * N :] = jnp.broadcast_to(rows, (8, H))


def stepped(obj, vel, g):
    vel = momentum_rate * vel + g
    return obj - step_size * vel, vel


def update_kernel(
    mask_ref, left_ref, right_ref, vel_ref, top_ref, bottom_ref, above_ref, before_ref,
    left_out, right_out, vl_out, vr_out, up_out, corner_out, send_out, fix_out,
):
    row_id = lax.broadcasted_iota(jnp.int32, (H, H), 0).astype(jnp.float32)
    ours_above = above_ref[2 * H : 2 * H + 1, :H] < 0.5
    ours_before = row_id >= before_ref[2 * N : 2 * N + 1]
    for part in range(2):
        above, before = above_ref[part * H : (part + 1) * H], before_ref[part * N : (part + 1) * N]
        g00 = (top_ref[part, :, :H] + jnp.where(ours_above, above[:, :H], 0.0)) + jnp.where(ours_before, before[:H], 0.0)
        g01 = top_ref[part, :, H:] + above[:, H:]
        g10 = bottom_ref[part, :, :H] + before[H:]
        g11 = bottom_ref[part, :, H:]
        obj, vel = stepped(left_ref[part, :H], vel_ref[part, :H, :H], g00)
        left_out[part, :H], vl_out[part, :H] = obj, vel
        up_out[part, :, :H], corner_out[part], send_out[part, :H] = obj, obj, obj
        obj, vel = stepped(right_ref[part, :H], vel_ref[part, :H, H:], g01)
        right_out[part, :H], vr_out[part, :H], up_out[part, :, H:] = obj, vel, obj
        obj, vel = stepped(left_ref[part, H:], vel_ref[part, H:, :H], g10)
        left_out[part, H:], vl_out[part, H:], send_out[part, H:] = obj, vel, obj
        right_out[part, H:], vr_out[part, H:] = stepped(right_ref[part, H:], vel_ref[part, H:, H:], g11)
        scale = mask_ref[2].astype(jnp.float32) * step_size
        fix_out[part, :, :H] = scale * jnp.where(ours_before, 0.0, before[:H])
        scale = mask_ref[3].astype(jnp.float32) * step_size
        fix_out[part, :, H:] = scale * jnp.where(ours_above, 0.0, above[:, :H])


def final_kernel(
    left_ref, right_ref, vl_ref, vr_ref, late_ref, top_ref, bottom_ref, above_ref, before_ref, diag_ref, obj_out, vel_out
):
    for part in range(2):
        g00 = (top_ref[part, :, :H] + above_ref[part, :, :H]) + (before_ref[part, :H] + diag_ref[part])
        g01 = top_ref[part, :, H:] + above_ref[part, :, H:]
        g10 = bottom_ref[part, :, :H] + before_ref[part, H:]
        g11 = bottom_ref[part, :, H:]
        obj = left_ref[part, :H] - step_size * late_ref[part]
        obj_out[part, :H, :H], vel_out[part, :H, :H] = stepped(obj, vl_ref[part, :H] + late_ref[part], g00)
        obj_out[part, H:, :H], vel_out[part, H:, :H] = stepped(left_ref[part, H:], vl_ref[part, H:], g10)
        for rows, g in ((slice(0, H), g01), (slice(H, N), g11)):
            obj_out[part, rows, H:], vel_out[part, rows, H:] = stepped(right_ref[part, rows], vr_ref[part, rows], g)


def shape(*dims, dtype=jnp.float32):
    return jax.ShapeDtypeStruct(dims, dtype)


def kernel(body, flops, scalars, arrays, outs):
    return pl.pallas_call(
        body,
        out_shape=outs,
        in_specs=[SMEM] * scalars + [VMEM] * arrays,
        out_specs=(VMEM,) * len(outs),
        compiler_params=pltpu.CompilerParams(vmem_limit_bytes=16 * 1024 * 1024),
        cost_estimate=pl.CostEstimate(flops=flops, bytes_accessed=10**6, transcendentals=0),
    )


def steps(object_field, velocity, positions, measured, probe):
    offsets = positions[0, 0, 0]
    intensity = measured[0, 0, 0]
    edges = [
        (lax.axis_index(axis) < lax.axis_size(axis) - 1).astype(jnp.int32).reshape(1) for axis in ("row", "col")
    ]
    half, strip, quad, rows = shape(2, N, H), shape(2, H, N), shape(2, H, H), shape(N, N)

    lower = shifted(object_field[:, :H, :], -1, 0)
    left, right, q00, left_send = kernel(unpack_kernel, 10**6, 0, 1, (half, half, quad, half))(object_field)
    beside = shifted(left_send, 0, -1)
    corner = shifted(q00, -1, -1)
    turned, intensity, mask, tables, along_cols, along_rows = kernel(
        prep_kernel, 10**8, 3, 2,
        (
            shape(2, N, N), rows, shape(4, H, H, dtype=jnp.int32),
            shape(4, N, N, dtype=jnp.bfloat16), shape(2, 8, H), shape(2, H, H),
        ),
    )(offsets, *edges, probe, intensity)

    def pre(left, right, beside):
        return kernel(pre_kernel, 10**8, 0, 7, (rows,))(
            mask, left, right, beside, turned, tables, along_cols
        )[0]

    def main(body, outs, *arrays):
        rest = (turned, intensity, pre(arrays[0], arrays[1], arrays[-2]), tables, along_cols, along_rows)
        return kernel(body, 10**9, 0, 1 + len(arrays) + len(rest), outs)(mask, *arrays, *rest)

    top, down, diag, r00, xb, kept = main(
        lambda *refs: main_kernel(True, *refs), (strip, shape(N + 8, N), quad, quad, rows, quad),
        left, right, lower, beside, corner,
    )
    above = shifted(down, 1, 0)
    bottom, right_part = kernel(post_kernel, 10**8, 0, 6, (strip, shape(2 * N + 8, H)))(
        mask, xb, r00, turned, tables, along_cols
    )
    before = shifted(right_part, 0, 1)
    late = shifted(diag, 1, 1)
    left, right, vel_left, vel_right, q00, q00_corner, left_send, fix = kernel(
        update_kernel, 10**6, 0, 8, (half, half, half, half, strip, quad, half, strip)
    )(mask, left, right, velocity, top, bottom, above, before)
    up00 = shifted(q00, -1, 0)
    corner = shifted(q00_corner, -1, -1)
    beside = shifted(left_send, 0, -1)
    top, down, diag, bottom, right_part = main(
        lambda *refs: main_kernel(False, *refs), (strip, strip, quad, strip, half),
        left, right, up00, kept, fix, late, beside, corner,
    )
    above = shifted(down, 1, 0)
    before = shifted(right_part, 0, 1)
    from_corner = shifted(diag, 1, 1)
    return kernel(final_kernel, 10**6, 0, 10, (shape(2, N, N), shape(2, N, N)))(
        left, right, vel_left, vel_right, late, top, bottom, above, before, from_corner
    )


def solution(mesh):
    placed = (
        P(None, "row", "col"),
        P(None, "row", "col"),
        P("row", "col", None, None),
        P("row", "col", None, None, None),
        P(),
    )
    return jax.shard_map(
        steps,
        mesh=mesh,
        in_specs=placed,
        out_specs=(P(None, "row", "col"), P(None, "row", "col")),
        check_vma=False,
    )
```

```python
import math

import jax
import jax.numpy as jnp
from jax import lax
from jax.experimental import pallas as pl
from jax.experimental.pallas import tpu as pltpu
from jax.sharding import PartitionSpec as P


P_SIZE = 256

step_size = 0.1
momentum_rate = 0.8

VMEM = pl.BlockSpec(memory_space=pltpu.VMEM)
SMEM = pl.BlockSpec(memory_space=pltpu.SMEM)
N = P_SIZE
H = P_SIZE // 2


def shifted(value, row_steps, col_steps):
    rows, cols = lax.axis_size("row"), lax.axis_size("col")
    pairs = []
    for r in range(rows):
        for c in range(cols):
            to_r, to_c = r + row_steps, c + col_steps
            if 0 <= to_r < rows and 0 <= to_c < cols:
                pairs.append((r * cols + c, to_r * cols + to_c))
    return lax.ppermute(value, ("row", "col"), pairs)


def turns(step, length, scale):
    step = jnp.where(step > length // 2, step - length, step)
    angle = step.astype(jnp.float32) * (-2.0 * math.pi / length)
    return jnp.cos(angle) * scale, jnp.sin(angle) * scale


def halves(x):
    high = x.astype(jnp.bfloat16)
    return high, (x - high.astype(jnp.float32)).astype(jnp.bfloat16)


def dot(a, b):
    return jnp.dot(a, b, preferred_element_type=jnp.float32)


def times(a, b):
    return dot(a[0], b[0]) + dot(a[0], b[1]) + dot(a[1], b[0])


def quads(q00, q01, q10, q11):
    return jnp.concatenate(
        [jnp.concatenate([q00, q01], axis=1), jnp.concatenate([q10, q11], axis=1)], axis=0
    )


def block_transpose(x):
    return quads(x[:H, :H], x[H:, :H], x[:H, H:], x[H:, H:])


def plus(table_ref):
    return table_ref[0], table_ref[1]


def minus(table_ref):
    return table_ref[2], table_ref[3]


def unpack_kernel(obj_ref, left_out, right_out, q00_out, send_out):
    for part in range(2):
        left_out[part] = obj_ref[part, :, :H]
        send_out[part] = obj_ref[part, :, :H]
        right_out[part] = obj_ref[part, :, H:]
        q00_out[part] = obj_ref[part, :H, :H]


def prep_kernel(
    pos_ref, below_ref, beside_ref, probe_ref, meas_ref, probe_out, meas_out, mask_out, table_out, cols_out, rows_out
):
    p0 = pos_ref[0]
    p1 = pos_ref[1]
    row_id = lax.broadcasted_iota(jnp.int32, (H, H), 0)
    col_id = lax.broadcasted_iota(jnp.int32, (H, H), 1)
    mask_out[0] = jnp.where(row_id < p0, 1, 0)
    mask_out[1] = jnp.where(col_id < p1, 1, 0)
    mask_out[2] = jnp.full((H, H), below_ref[0], jnp.int32)
    mask_out[3] = jnp.full((H, H), beside_ref[0], jnp.int32)
    c, s = turns(row_id * col_id & (H - 1), H, 1.0 / math.sqrt(P_SIZE))
    for number, block in enumerate((quads(c, s, -s, c), quads(c, -s, s, c))):
        table_out[2 * number], table_out[2 * number + 1] = halves(block)
    rows_out[0], rows_out[1] = turns(row_id, P_SIZE, 1.0)
    cols_out[0], cols_out[1] = turns(col_id[:8], P_SIZE, 1.0)
    for part in range(2):
        x = pltpu.roll(probe_ref[part], p0, 0)
        probe_out[part] = pltpu.roll(x, p1, 1)
    first = lax.broadcasted_iota(jnp.int32, (N, N), 0)
    second = lax.broadcasted_iota(jnp.int32, (N, N), 1)

    def evens_first(place):
        return jnp.where(place < H, 2 * place, 2 * (place - H) + 1)

    def moved(x, move):
        high, rest = halves(x)
        mid = x - high.astype(jnp.float32)
        low = (mid - rest.astype(jnp.float32)).astype(jnp.bfloat16)
        return move(high) + (move(rest) + move(low))

    rows_move = jnp.where(second == evens_first(first), 1.0, 0.0).astype(jnp.bfloat16)
    cols_move = jnp.where(first == evens_first(second), 1.0, 0.0).astype(jnp.bfloat16)
    x = moved(meas_ref[...], lambda part: dot(rows_move, part))
    meas_out[...] = moved(x, lambda part: dot(part, cols_move))


def row_stage(patch, pr, pi, table, w_ref):
    er = pr * patch[0] - pi * patch[1]
    ei = pr * patch[1] + pi * patch[0]
    wr, wi = w_ref[0, 0:1], w_ref[1, 0:1]
    dr, di = er[:, :H] - er[:, H:], ei[:, :H] - ei[:, H:]
    x = quads(
        er[:, :H] + er[:, H:], ei[:, :H] + ei[:, H:], dr * wr - di * wi, dr * wi + di * wr
    )
    return times(halves(x), table)


def back_stage(x, pr, pi, table, w_ref):
    y = times(halves(block_transpose(x)), table)
    wr, wi = w_ref[0, 0:1], w_ref[1, 0:1]
    qr, qi = y[H:, :H], y[H:, H:]
    tr, ti = qr * wr + qi * wi, qi * wr - qr * wi
    br = jnp.concatenate([y[:H, :H] + tr, y[:H, :H] - tr], axis=1)
    bi = jnp.concatenate([y[:H, H:] + ti, y[:H, H:] - ti], axis=1)
    return pr * br + pi * bi, pr * bi - pi * br


def masks(mask_ref):
    return mask_ref[0] > 0, mask_ref[1] > 0


def pre_kernel(mask_ref, left_ref, right_ref, beside_ref, probe_ref, table_ref, cols_ref, y_ref):
    _, beyond = masks(mask_ref)
    patch = [
        jnp.concatenate(
            [jnp.where(beyond, beside_ref[part, H:], left_ref[part, H:]), right_ref[part, H:]], axis=1
        )
        for part in range(2)
    ]
    y_ref[...] = row_stage(patch, probe_ref[0, H:], probe_ref[1, H:], plus(table_ref), cols_ref)


def main_kernel(first, *refs):
    if first:
        (mask_ref, left_ref, right_ref, lower_ref, beside_ref, corner_ref, probe_ref, meas_ref, yb_ref,
         table_ref, cols_ref, rows_ref, own_out, down_out, diag_out, r00_out, xb_out, kept_out) = refs
    else:
        (mask_ref, left_ref, right_ref, up_ref, kept_ref, fix_ref, diag_ref, beside_ref, corner_ref,
         probe_ref, meas_ref, yb_ref, table_ref, cols_ref, rows_ref,
         own_out, down_out, diag_out, bottom_out, right_out) = refs
        corner_scale = (mask_ref[2] * mask_ref[3]).astype(jnp.float32) * step_size
    below, beyond = masks(mask_ref)
    pr, pi = probe_ref[0, :H], probe_ref[1, :H]
    patch = []
    for part in range(2):
        own00, beside = left_ref[part, :H], beside_ref[part, :H]
        if first:
            lower00, lower01, corner = lower_ref[part, :, :H], lower_ref[part, :, H:], corner_ref[part]
        else:
            own00 = own00 - step_size * diag_ref[part]
            beside = beside - fix_ref[part, :, H:]
            lower00 = up_ref[part, :, :H] - fix_ref[part, :, :H]
            lower01 = up_ref[part, :, H:]
            corner = corner_ref[part] - corner_scale * kept_ref[part]
        q00 = jnp.where(below, jnp.where(beyond, corner, lower00), jnp.where(beyond, beside, own00))
        q01 = jnp.where(below, lower01, right_ref[part, :H])
        patch.append(jnp.concatenate([q00, q01], axis=1))
    yt = row_stage(patch, pr, pi, plus(table_ref), cols_ref)
    yb = yb_ref[...]
    wr = jnp.concatenate([rows_ref[0], rows_ref[0]], axis=0)
    wi = jnp.concatenate([rows_ref[1], rows_ref[1]], axis=0)
    diff = yt - yb
    dr, di = diff[:, :H], diff[:, H:]
    odd = jnp.concatenate([dr * wr - di * wi, dr * wi + di * wr], axis=1)
    back = []
    for parity, x in enumerate((yt + yb, odd)):
        z = times(minus(table_ref), halves(block_transpose(x)))
        zr, zi = z[:H], z[H:]
        misfit = zr * zr + zi * zi - meas_ref[parity * H : (parity + 1) * H]
        g = jnp.concatenate([misfit * zr, misfit * zi], axis=0)
        back.append(times(plus(table_ref), halves(g)))
    qr, qi = back[1][:H], back[1][H:]
    wr = jnp.concatenate([rows_ref[0], rows_ref[0]], axis=1)
    wi = jnp.concatenate([rows_ref[1], rows_ref[1]], axis=1)
    turned = jnp.concatenate([qr * wr + qi * wi, qi * wr - qr * wi], axis=0)
    if first:
        xb_out[...] = back[0] - turned
    out = back_stage(back[0] + turned, pr, pi, minus(table_ref), cols_ref)
    for part in range(2):
        g00, g01 = out[part][:, :H], out[part][:, H:]
        own_out[part, :, :H] = jnp.where(jnp.logical_or(below, beyond), 0.0, g00)
        own_out[part, :, H:] = jnp.where(below, 0.0, g01)
        d01 = jnp.where(below, g01, 0.0)
        diag = jnp.where(jnp.logical_and(below, beyond), g00, 0.0)
        diag_out[part] = diag
        if first:
            down_out[part * H : (part + 1) * H, :H] = jnp.where(below, g00, 0.0)
            down_out[part * H : (part + 1) * H, H:] = d01
            r00_out[part] = jnp.where(beyond, g00, 0.0)
            kept_out[part] = diag
        else:
            down_out[part, :, :H] = jnp.where(jnp.logical_and(below, ~beyond), g00, 0.0)
            down_out[part, :, H:] = d01
            right_out[part, :H] = jnp.where(jnp.logical_and(~below, beyond), g00, 0.0)
    if first:
        down_out[2 * H :, :H] = mask_ref[1, :8].astype(jnp.float32)
        down_out[2 * H :, H:] = jnp.zeros((8, H), jnp.float32)
    else:
        out = back_stage(back[0] - turned, probe_ref[0, H:], probe_ref[1, H:], minus(table_ref), cols_ref)
        for part in range(2):
            g10, g11 = out[part][:, :H], out[part][:, H:]
            bottom_out[part, :, :H] = jnp.where(beyond, 0.0, g10)
            bottom_out[part, :, H:] = g11
            right_out[part, H:] = jnp.where(beyond, g10, 0.0)


def post_kernel(mask_ref, xb_ref, r00_ref, probe_ref, table_ref, cols_ref, own_out, right_out):
    below, beyond = masks(mask_ref)
    out = back_stage(xb_ref[...], probe_ref[0, H:], probe_ref[1, H:], minus(table_ref), cols_ref)
    for part in range(2):
        g10, g11 = out[part][:, :H], out[part][:, H:]
        own_out[part, :, :H] = jnp.where(beyond, 0.0, g10)
        own_out[part, :, H:] = g11
        right_out[part * N : part * N + H] = r00_ref[part]
        right_out[part * N + H : (part + 1) * N] = jnp.where(beyond, g10, 0.0)
    rows = jnp.sum(below.astype(jnp.float32), axis=0, keepdims=True)
    right_out[2 * N :] = jnp.broadcast_to(rows, (8, H))


def stepped(obj, vel, g):
    vel = momentum_rate * vel + g
    return obj - step_size * vel, vel


def arrived(above_ref, before_ref):
    row_id = lax.broadcasted_iota(jnp.int32, (H, H), 0).astype(jnp.float32)
    return above_ref[2 * H : 2 * H + 1, :H] < 0.5, row_id >= before_ref[2 * N : 2 * N + 1]


def gradients(part, masks_of, top_ref, bottom_ref, above_ref, before_ref):
    ours_above, ours_before = masks_of
    above, before = above_ref[part * H : (part + 1) * H], before_ref[part * N : (part + 1) * N]
    g00 = (top_ref[part, :, :H] + jnp.where(ours_above, above[:, :H], 0.0)) + jnp.where(ours_before, before[:H], 0.0)
    return g00, top_ref[part, :, H:] + above[:, H:], bottom_ref[part, :, :H] + before[H:], bottom_ref[part, :, H:]


def send_kernel(left_ref, right_ref, vel_ref, top_ref, bottom_ref, above_ref, before_ref, up_out, corner_out, send_out):
    ours = arrived(above_ref, before_ref)
    for part in range(2):
        g00, g01, g10, _ = gradients(part, ours, top_ref, bottom_ref, above_ref, before_ref)
        obj, _ = stepped(left_ref[part, :H], vel_ref[part, :H, :H], g00)
        up_out[part, :, :H], corner_out[part], send_out[part, :H] = obj, obj, obj
        up_out[part, :, H:], _ = stepped(right_ref[part, :H], vel_ref[part, :H, H:], g01)
        send_out[part, H:], _ = stepped(left_ref[part, H:], vel_ref[part, H:, :H], g10)


def update_kernel(
    mask_ref, left_ref, right_ref, vel_ref, top_ref, bottom_ref, above_ref, before_ref,
    left_out, right_out, vl_out, vr_out, fix_out,
):
    ours_above, ours_before = ours = arrived(above_ref, before_ref)
    for part in range(2):
        g00, g01, g10, g11 = gradients(part, ours, top_ref, bottom_ref, above_ref, before_ref)
        left_out[part, :H], vl_out[part, :H] = stepped(left_ref[part, :H], vel_ref[part, :H, :H], g00)
        left_out[part, H:], vl_out[part, H:] = stepped(left_ref[part, H:], vel_ref[part, H:, :H], g10)
        right_out[part, :H], vr_out[part, :H] = stepped(right_ref[part, :H], vel_ref[part, :H, H:], g01)
        right_out[part, H:], vr_out[part, H:] = stepped(right_ref[part, H:], vel_ref[part, H:, H:], g11)
        scale = mask_ref[2].astype(jnp.float32) * step_size
        fix_out[part, :, :H] = scale * jnp.where(ours_before, 0.0, before_ref[part * N : part * N + H])
        scale = mask_ref[3].astype(jnp.float32) * step_size
        fix_out[part, :, H:] = scale * jnp.where(ours_above, 0.0, above_ref[part * H : (part + 1) * H, :H])


def final_kernel(
    left_ref, right_ref, vl_ref, vr_ref, late_ref, top_ref, bottom_ref, above_ref, before_ref, diag_ref, obj_out, vel_out
):
    for part in range(2):
        g00 = (top_ref[part, :, :H] + above_ref[part, :, :H]) + (before_ref[part, :H] + diag_ref[part])
        g01 = top_ref[part, :, H:] + above_ref[part, :, H:]
        g10 = bottom_ref[part, :, :H] + before_ref[part, H:]
        g11 = bottom_ref[part, :, H:]
        obj = left_ref[part, :H] - step_size * late_ref[part]
        obj_out[part, :H, :H], vel_out[part, :H, :H] = stepped(obj, vl_ref[part, :H] + late_ref[part], g00)
        obj_out[part, H:, :H], vel_out[part, H:, :H] = stepped(left_ref[part, H:], vl_ref[part, H:], g10)
        for rows, g in ((slice(0, H), g01), (slice(H, N), g11)):
            obj_out[part, rows, H:], vel_out[part, rows, H:] = stepped(right_ref[part, rows], vr_ref[part, rows], g)


def shape(*dims, dtype=jnp.float32):
    return jax.ShapeDtypeStruct(dims, dtype)


def kernel(body, flops, scalars, arrays, outs):
    return pl.pallas_call(
        body,
        out_shape=outs,
        in_specs=[SMEM] * scalars + [VMEM] * arrays,
        out_specs=(VMEM,) * len(outs),
        compiler_params=pltpu.CompilerParams(vmem_limit_bytes=16 * 1024 * 1024),
        cost_estimate=pl.CostEstimate(flops=flops, bytes_accessed=10**6, transcendentals=0),
    )


def steps(object_field, velocity, positions, measured, probe):
    offsets = positions[0, 0, 0]
    intensity = measured[0, 0, 0]
    edges = [
        (lax.axis_index(axis) < lax.axis_size(axis) - 1).astype(jnp.int32).reshape(1) for axis in ("row", "col")
    ]
    half, strip, quad, rows = shape(2, N, H), shape(2, H, N), shape(2, H, H), shape(N, N)

    lower = shifted(object_field[:, :H, :], -1, 0)
    left, right, q00, left_send = kernel(unpack_kernel, 10**6, 0, 1, (half, half, quad, half))(object_field)
    beside = shifted(left_send, 0, -1)
    corner = shifted(q00, -1, -1)
    turned, intensity, mask, tables, along_cols, along_rows = kernel(
        prep_kernel, 10**8, 3, 2,
        (
            shape(2, N, N), rows, shape(4, H, H, dtype=jnp.int32),
            shape(4, N, N, dtype=jnp.bfloat16), shape(2, 8, H), shape(2, H, H),
        ),
    )(offsets, *edges, probe, intensity)

    def pre(left, right, beside):
        return kernel(pre_kernel, 10**8, 0, 7, (rows,))(
            mask, left, right, beside, turned, tables, along_cols
        )[0]

    def main(body, outs, *arrays):
        rest = (turned, intensity, pre(arrays[0], arrays[1], arrays[-2]), tables, along_cols, along_rows)
        return kernel(body, 10**9, 0, 1 + len(arrays) + len(rest), outs)(mask, *arrays, *rest)

    top, down, diag, r00, xb, kept = main(
        lambda *refs: main_kernel(True, *refs), (strip, shape(N + 8, N), quad, quad, rows, quad),
        left, right, lower, beside, corner,
    )
    above = shifted(down, 1, 0)
    bottom, right_part = kernel(post_kernel, 10**8, 0, 6, (strip, shape(2 * N + 8, H)))(
        mask, xb, r00, turned, tables, along_cols
    )
    before = shifted(right_part, 0, 1)
    late = shifted(diag, 1, 1)
    up_send, q00, left_send = kernel(send_kernel, 10**6, 0, 7, (strip, quad, half))(
        left, right, velocity, top, bottom, above, before
    )
    lower = shifted(up_send, -1, 0)
    beside = shifted(left_send, 0, -1)
    corner = shifted(q00, -1, -1)
    left, right, vel_left, vel_right, fix = kernel(
        update_kernel, 10**6, 0, 8, (half, half, half, half, strip)
    )(mask, left, right, velocity, top, bottom, above, before)
    top, down, diag, bottom, right_part = main(
        lambda *refs: main_kernel(False, *refs), (strip, strip, quad, strip, half),
        left, right, lower, kept, fix, late, beside, corner,
    )
    above = shifted(down, 1, 0)
    before = shifted(right_part, 0, 1)
    from_corner = shifted(diag, 1, 1)
    return kernel(final_kernel, 10**6, 0, 10, (shape(2, N, N), shape(2, N, N)))(
        left, right, vel_left, vel_right, late, top, bottom, above, before, from_corner
    )


def solution(mesh):
    placed = (
        P(None, "row", "col"),
        P(None, "row", "col"),
        P("row", "col", None, None),
        P("row", "col", None, None, None),
        P(),
    )
    return jax.shard_map(
        steps,
        mesh=mesh,
        in_specs=placed,
        out_specs=(P(None, "row", "col"), P(None, "row", "col")),
        check_vma=False,
    )
```
